32 devices in a mesh: dp: 2 (over x), tp: 4 (over z), sp: 4 (over y, core).
Axes of the slice: x: 2, y: 2, z: 4, core: 2. Of those that a mesh axis runs over, the one named last changes fastest.
Arguments:
- tokens: bfloat16 [16, 3584], P('dp'), parts along dimension 0
- positions: int32 [16], P('dp'), parts along dimension 0
- cache_k: bfloat16 [16, 4096, 8, 256], P('dp', 'sp', 'tp'), parts along dimension 0
- cache_v: bfloat16 [16, 4096, 8, 256], P('dp', 'sp', 'tp'), parts along dimension 0
- attn_gain: bfloat16 [3584], replicated
- w_q: bfloat16 [3584, 4096], P(None, 'tp')
- w_k: bfloat16 [3584, 2048], P(None, 'tp')
- w_v: bfloat16 [3584, 2048], P(None, 'tp')
- w_o: bfloat16 [4096, 3584], P('tp')
- mlp_gain: bfloat16 [3584], replicated
- w_gate: bfloat16 [3584, 14336], P(None, 'tp')
- w_up: bfloat16 [3584, 14336], P(None, 'tp')
- w_down: bfloat16 [14336, 3584], P('tp')
Outputs:
- output 1: bfloat16 [16, 3584], P('dp'), parts along dimension 0
- output 2: bfloat16 [16, 4096, 8, 256], P('dp', 'sp', 'tp'), parts along dimension 0
- output 3: bfloat16 [16, 4096, 8, 256], P('dp', 'sp', 'tp'), parts along dimension 0
There are 2 independent parts. The reference program is written for one: setup_inputs(seed, part) draws one part's arguments, and reference() takes and returns one part's arrays. A program takes and returns all parts, laid end to end along the dimension named above; an argument that names none is the same for every part.
All inputs are finite; a program needn't handle non-finite values.
Results may differ from the reference program's by a relative error of at most 0.0088623.
Values sent between devices are 32-bit elements.
A program may use at most 1 GiB of HBM per device.

```python
import math
import jax
import jax.numpy as jnp
from jax import lax

BATCH = 8
MODEL_DIM = 3584
HEADS = 16
KV_HEADS = 8
HEAD_DIM = 256
MLP_DIM = 14336
SLOTS = 4096
GROUP = HEADS // KV_HEADS
POS_LIMIT = 8 * SLOTS
LOG_SLOTS = int(math.log2(SLOTS))
NORM_EPS = 1e-5
ROPE_THETA = 10000.0
KEY_STD = math.sqrt(math.log(SLOTS / 8.0))
VALUE_STD = 1.5


def draw_positions(key):
    rank_key, scale_key, young_key, old_key = jax.random.split(key, 4)
    order = jax.random.permutation(rank_key, BATCH)
    is_young = order < BATCH // 2
    exponent = jax.random.randint(scale_key, (BATCH,), 0, LOG_SLOTS + 1)
    limit = jnp.minimum(jnp.left_shift(jnp.ones_like(exponent), exponent), SLOTS)
    young_pos = jax.random.randint(young_key, (BATCH,), 0, limit)
    old_pos = jax.random.randint(old_key, (BATCH,), SLOTS, POS_LIMIT)
    return jnp.where(is_young, young_pos, old_pos).astype(jnp.int32)


def normal_matrix(key, rows, columns, scale):
    return (jax.random.normal(key, (rows, columns), jnp.float32) * scale).astype(jnp.bfloat16)


def normal_gain(key):
    return (1.0 + 0.3 * jax.random.normal(key, (MODEL_DIM,), jnp.float32)).astype(jnp.bfloat16)


def setup_inputs(seed: int = 0, part: int = 0) -> dict:
    base_key = jax.random.key(seed)
    part_keys = jax.random.split(jax.random.fold_in(base_key, part), 4)
    weight_keys = jax.random.split(base_key, 9)
    cache_shape = (BATCH, SLOTS, KV_HEADS, HEAD_DIM)
    query_width = HEADS * HEAD_DIM
    kv_width = KV_HEADS * HEAD_DIM
    tokens = jax.random.normal(part_keys[0], (BATCH, MODEL_DIM), jnp.float32).astype(jnp.bfloat16)
    positions = draw_positions(part_keys[1])
    cache_k = (KEY_STD * jax.random.normal(part_keys[2], cache_shape, jnp.float32)).astype(jnp.bfloat16)
    cache_v = (VALUE_STD * jax.random.normal(part_keys[3], cache_shape, jnp.float32)).astype(jnp.bfloat16)
    return {
        "tokens": tokens,
        "positions": positions,
        "cache_k": cache_k,
        "cache_v": cache_v,
        "attn_gain": normal_gain(weight_keys[0]),
        "w_q": normal_matrix(weight_keys[1], MODEL_DIM, query_width, MODEL_DIM ** -0.5),
        "w_k": normal_matrix(weight_keys[2], MODEL_DIM, kv_width, KEY_STD * MODEL_DIM ** -0.5),
        "w_v": normal_matrix(weight_keys[3], MODEL_DIM, kv_width, VALUE_STD * MODEL_DIM ** -0.5),
        "w_o": normal_matrix(weight_keys[4], query_width, MODEL_DIM, query_width ** -0.5),
        "mlp_gain": normal_gain(weight_keys[5]),
        "w_gate": normal_matrix(weight_keys[6], MODEL_DIM, MLP_DIM, MODEL_DIM ** -0.5),
        "w_up": normal_matrix(weight_keys[7], MODEL_DIM, MLP_DIM, MODEL_DIM ** -0.5),
        "w_down": normal_matrix(weight_keys[8], MLP_DIM, MODEL_DIM, MLP_DIM ** -0.5),
    }


def rms_norm(values, gain):
    wide = values.astype(jnp.float32)
    inv_rms = lax.rsqrt(jnp.mean(wide * wide, axis=-1, keepdims=True) + NORM_EPS)
    return (wide * inv_rms * gain.astype(jnp.float32)).astype(jnp.bfloat16)


def rope_tables(positions):
    frequencies = ROPE_THETA ** (-2.0 * jnp.arange(HEAD_DIM // 2, dtype=jnp.float32) / HEAD_DIM)
    angles = positions.astype(jnp.float32)[:, None] * frequencies[None, :]
    return jnp.cos(angles)[:, None, :], jnp.sin(angles)[:, None, :]


def apply_rope(vectors, cos_table, sin_table):
    half = vectors.shape[-1] // 2
    first = vectors[..., :half]
    second = vectors[..., half:]
    return jnp.concatenate([first * cos_table - second * sin_table, second * cos_table + first * sin_table], axis=-1)


def reference(tokens, positions, cache_k, cache_v, attn_gain, w_q, w_k, w_v, w_o, mlp_gain, w_gate, w_up, w_down):
    normed = rms_norm(tokens, attn_gain)
    cos_table, sin_table = rope_tables(positions)
    q_lin = jnp.dot(normed, w_q, preferred_element_type=jnp.float32).reshape(BATCH, HEADS, HEAD_DIM)
    k_lin = jnp.dot(normed, w_k, preferred_element_type=jnp.float32).reshape(BATCH, KV_HEADS, HEAD_DIM)
    v_new = jnp.dot(normed, w_v, preferred_element_type=jnp.float32).astype(jnp.bfloat16).reshape(BATCH, KV_HEADS, HEAD_DIM)
    q_rot = apply_rope(q_lin, cos_table, sin_table).astype(jnp.bfloat16)
    k_rot = apply_rope(k_lin, cos_table, sin_table).astype(jnp.bfloat16)
    slot_ids = jnp.arange(SLOTS)
    hit_mask = (slot_ids[None, :] == (positions % SLOTS)[:, None])[:, :, None, None]
    new_k = jnp.where(hit_mask, k_rot[:, None], cache_k)
    new_v = jnp.where(hit_mask, v_new[:, None], cache_v)

    def attend_one(item):
        q_seq, k_seq, v_seq, pos_one = item
        query = q_seq.astype(jnp.float32).reshape(KV_HEADS, GROUP, HEAD_DIM)
        scores = jnp.einsum("kgd,skd->kgs", query, k_seq.astype(jnp.float32)) / math.sqrt(HEAD_DIM)
        valid = (pos_one >= SLOTS - 1) | (slot_ids <= pos_one)
        scores = jnp.where(valid[None, None, :], scores, -jnp.inf)
        weights = jax.nn.softmax(scores, axis=-1)
        return jnp.einsum("kgs,skd->kgd", weights, v_seq.astype(jnp.float32)).reshape(HEADS, HEAD_DIM)

    attended = lax.map(attend_one, (q_rot, new_k, new_v, positions))
    attended = attended.reshape(BATCH, HEADS * HEAD_DIM).astype(jnp.bfloat16)
    attn_proj = jnp.dot(attended, w_o, preferred_element_type=jnp.float32)
    hidden = (tokens.astype(jnp.float32) + attn_proj).astype(jnp.bfloat16)
    normed_mlp = rms_norm(hidden, mlp_gain)
    gate_proj = jnp.dot(normed_mlp, w_gate, preferred_element_type=jnp.float32)
    up_proj = jnp.dot(normed_mlp, w_up, preferred_element_type=jnp.float32)
    activated = (jax.nn.silu(gate_proj) * up_proj).astype(jnp.bfloat16)
    mlp_down = jnp.dot(activated, w_down, preferred_element_type=jnp.float32)
    layer_out = (hidden.astype(jnp.float32) + mlp_down).astype(jnp.bfloat16)
    return (layer_out, new_k, new_v)
```

```python
import math
import functools
import jax
import jax.numpy as jnp
from jax import lax
from jax.experimental import pallas as pl
from jax.experimental.pallas import tpu as pltpu
from jax.sharding import PartitionSpec as P

NORM_EPS = 1e-5
ROPE_THETA = 10000.0
MESH = pl.DeviceIdType.MESH
F32 = jnp.float32
BF16 = jnp.bfloat16


def rms_norm(wide, gain):
    inv_rms = lax.rsqrt(jnp.mean(wide * wide, axis=-1, keepdims=True) + NORM_EPS)
    return (wide * inv_rms * gain.astype(F32)).astype(BF16)


def rope_tables(positions, head_dim):
    frequencies = ROPE_THETA ** (-2.0 * jnp.arange(head_dim // 2, dtype=F32) / head_dim)
    angles = positions.astype(F32)[:, None] * frequencies[None, :]
    return jnp.cos(angles), jnp.sin(angles)


def attention_kernel(sp_size, chunks, pos_ref, tok_ref, gain_ref, cos_ref, sin_ref, wq, wk, wv, ck, cv,
                     new_k, new_v, packed_ref,
                     wbuf, kbuf, vbuf, q3, k3, v3, o3, m3, l3, wsem, ksem, vsem, okm, ovm):
    rows, local_slots, kv_local, head_dim = kbuf.shape
    slots = local_slots * sp_size
    depth = tok_ref.shape[1]
    q_width, kv_width = wq.shape[1], wk.shape[1]
    heads = q_width // head_dim
    group = heads // kv_local
    half = head_dim // 2
    step = depth // chunks
    first_slot = lax.axis_index("sp") * local_slots

    weight_copies = []
    for c in range(chunks):
        part = pl.ds(c * step, step)
        trio = [
            pltpu.make_async_copy(wq.at[part, :], wbuf.at[part, pl.ds(0, q_width)], wsem.at[c, 0]),
            pltpu.make_async_copy(wk.at[part, :], wbuf.at[part, pl.ds(q_width, kv_width)], wsem.at[c, 1]),
            pltpu.make_async_copy(wv.at[part, :], wbuf.at[part, pl.ds(q_width + kv_width, kv_width)], wsem.at[c, 2]),
        ]
        for copy in trio:
            copy.start()
        weight_copies.append(trio)
    k_in, v_in = [], []
    for b in range(rows):
        k_in.append(pltpu.make_async_copy(ck.at[b], kbuf.at[b], ksem.at[b]))
        v_in.append(pltpu.make_async_copy(cv.at[b], vbuf.at[b], vsem.at[b]))
        k_in[b].start()
        v_in[b].start()

    normed = rms_norm(tok_ref[...].astype(F32), gain_ref[...])
    acc = jnp.zeros((rows, q_width + 2 * kv_width), F32)
    for c in range(chunks):
        for copy in weight_copies[c]:
            copy.wait()
        acc = acc + jnp.dot(normed[:, c * step:(c + 1) * step], wbuf[c * step:(c + 1) * step, :], preferred_element_type=F32)

    cos_table, sin_table = cos_ref[...], sin_ref[...]
    scale = 1.0 / math.sqrt(head_dim)

    def rotate(start):
        a = acc[:, start:start + half]
        b = acc[:, start + half:start + head_dim]
        return a * cos_table - b * sin_table, b * cos_table + a * sin_table

    for j in range(heads):
        a, b = rotate(j * head_dim)
        q3[:, j, 0:half] = a
        q3[:, j, half:head_dim] = b
    for j in range(kv_local):
        a, b = rotate(q_width + j * head_dim)
        k3[:, j, 0:half] = a
        k3[:, j, half:head_dim] = b
        start = q_width + kv_width + j * head_dim
        v3[:, j, :] = acc[:, start:start + head_dim]

    width = local_slots * kv_local
    column = lax.broadcasted_iota(jnp.int32, (heads, width), 1)
    own_head = lax.rem(column, kv_local) == lax.broadcasted_iota(jnp.int32, (heads, width), 0) // group
    slot_ids = first_slot + column // kv_local
    k_out, v_out = [], []
    for b in range(rows):
        position = pos_ref[b]
        target = lax.rem(position, slots) - first_slot
        k_in[b].wait()
        v_in[b].wait()

        @pl.when((target >= 0) & (target < local_slots))
        def _():
            kbuf[b, target] = k3[b].astype(BF16)
            vbuf[b, target] = v3[b].astype(BF16)

        q_b = q3[b].astype(BF16)
        keys = kbuf[b].reshape(width, head_dim)
        scores = lax.dot_general(q_b, keys, (((1,), (1,)), ((), ())), preferred_element_type=F32) * scale
        limit = jnp.where(position >= slots - 1, slots, position)
        valid = own_head & (slot_ids <= limit)
        scores = jnp.where(valid, scores, -jnp.inf)
        top = jnp.max(scores, axis=1, keepdims=True)
        weights = jnp.where(valid, jnp.exp(scores - top), 0.0)
        k_out.append(pltpu.make_async_copy(kbuf.at[b], new_k.at[b], okm.at[b]))
        v_out.append(pltpu.make_async_copy(vbuf.at[b], new_v.at[b], ovm.at[b]))
        k_out[b].start()
        v_out[b].start()
        o3[b] = jnp.dot(weights.astype(BF16), vbuf[b].reshape(width, head_dim), preferred_element_type=F32)
        m3[b] = jnp.broadcast_to(top, (heads, 128))
        l3[b] = jnp.broadcast_to(jnp.sum(weights, axis=1, keepdims=True), (heads, 128))

    lane = lax.broadcasted_iota(jnp.int32, (rows, 128), 1) // 16
    stats = jnp.zeros((rows, 128), F32)
    for j in range(heads):
        packed_ref[:, j * head_dim:(j + 1) * head_dim] = o3[:, j, :]
        stats = jnp.where(lane == j, m3[:, j, :], stats)
        stats = jnp.where(lane == heads + j, l3[:, j, :], stats)
    packed_ref[:, q_width:q_width + 128] = stats
    for b in range(rows):
        k_out[b].wait()
        v_out[b].wait()


def exchange(axis, source, slots_ref, send_sem, recv_sem):
    me = lax.axis_index(axis)
    size = slots_ref.shape[0]
    copies = []
    for d in range(1, size):
        copy = pltpu.make_async_remote_copy(
            src_ref=source, dst_ref=slots_ref.at[me], send_sem=send_sem.at[d - 1], recv_sem=recv_sem.at[d - 1],
            device_id={axis: lax.rem(me + d, size)}, device_id_type=MESH)
        copy.start()
        copies.append(copy)
    return copies


def finish(copies):
    for copy in copies:
        copy.wait()


def mlp_kernel(head_dim, packed_ref, tok_ref, gain_ref, wo, wg, wu, wd, out_ref,
               wo_buf, wgu_buf, wd_buf, r1, part2, r2, part3, r3, part4, r4, part5, r5, part6, r6,
               wsem, ssem, rsem):
    rows, depth = tok_ref.shape
    sp_size, tp_size = r1.shape[0], r2.shape[0]
    q_width = wo.shape[0]
    heads = q_width // head_dim
    width = depth // sp_size
    hidden_width = wg.shape[1] // sp_size
    sp = lax.axis_index("sp")
    tp = lax.axis_index("tp")
    my_cols = pl.ds(pl.multiple_of(sp * width, 128), width)
    my_hidden = pl.ds(pl.multiple_of(sp * hidden_width, 128), hidden_width)

    barrier = pltpu.get_barrier_semaphore()
    for axis, me, size in (("sp", sp, sp_size), ("tp", tp, tp_size)):
        for d in range(1, size):
            pl.semaphore_signal(barrier, inc=1, device_id={axis: lax.rem(me + d, size)}, device_id_type=MESH)
    loads = [
        pltpu.make_async_copy(wo.at[:, my_cols], wo_buf, wsem.at[0]),
        pltpu.make_async_copy(wg.at[:, my_hidden], wgu_buf.at[:, pl.ds(0, hidden_width)], wsem.at[1]),
        pltpu.make_async_copy(wu.at[:, my_hidden], wgu_buf.at[:, pl.ds(hidden_width, hidden_width)], wsem.at[2]),
        pltpu.make_async_copy(wd.at[:, my_cols], wd_buf, wsem.at[3]),
    ]
    for copy in loads:
        copy.start()
    pl.semaphore_wait(barrier, sp_size + tp_size - 2)

    copies = exchange("sp", packed_ref, r1, ssem.at[0], rsem.at[0])
    r1[sp] = packed_ref[...]
    loads[0].wait()
    finish(copies)
    stats = [r1[s, :, q_width:q_width + 128] for s in range(sp_size)]
    pieces = []
    for j in range(heads):
        tops = [t[:, j * 16:j * 16 + 1] for t in stats]
        best = functools.reduce(jnp.maximum, tops)
        numerator = jnp.zeros((rows, head_dim), F32)
        denominator = jnp.zeros((rows, 1), F32)
        for s in range(sp_size):
            factor = jnp.exp(tops[s] - best)
            numerator = numerator + r1[s, :, j * head_dim:(j + 1) * head_dim] * factor
            denominator = denominator + stats[s][:, (heads + j) * 16:(heads + j) * 16 + 1] * factor
        pieces.append((numerator / denominator).astype(BF16))
    attended = jnp.concatenate(pieces, axis=1)
    part2[...] = jnp.dot(attended, wo_buf[...], preferred_element_type=F32)

    copies = exchange("tp", part2, r2, ssem.at[1], rsem.at[1])
    r2[tp] = part2[...]
    tokens_chunk = tok_ref[:, my_cols].astype(F32)
    finish(copies)
    total = r2[0]
    for t in range(1, tp_size):
        total = total + r2[t]
    hidden_chunk = (tokens_chunk + total).astype(BF16).astype(F32)
    part3[...] = hidden_chunk

    copies = exchange("sp", part3, r3, ssem.at[2], rsem.at[2])
    r3[sp] = hidden_chunk
    loads[1].wait()
    loads[2].wait()
    finish(copies)
    hidden = jnp.concatenate([r3[s] for s in range(sp_size)], axis=1)
    normed = rms_norm(hidden, gain_ref[...])
    both = jnp.dot(normed, wgu_buf[...], preferred_element_type=F32)
    gate, up = both[:, :hidden_width], both[:, hidden_width:]
    active = (gate * jax.nn.sigmoid(gate) * up).astype(BF16).astype(F32)
    part4[...] = active

    copies = exchange("sp", part4, r4, ssem.at[3], rsem.at[3])
    r4[sp] = active
    loads[3].wait()
    finish(copies)
    activated = jnp.concatenate([r4[s] for s in range(sp_size)], axis=1).astype(BF16)
    part5[...] = jnp.dot(activated, wd_buf[...], preferred_element_type=F32)

    copies = exchange("tp", part5, r5, ssem.at[4], rsem.at[4])
    r5[tp] = part5[...]
    finish(copies)
    total = r5[0]
    for t in range(1, tp_size):
        total = total + r5[t]
    out_chunk = (hidden_chunk + total).astype(BF16).astype(F32)
    part6[...] = out_chunk

    copies = exchange("sp", part6, r6, ssem.at[5], rsem.at[5])
    r6[sp] = out_chunk
    finish(copies)
    out_ref[...] = jnp.concatenate([r6[s] for s in range(sp_size)], axis=1).astype(BF16)


def solution(mesh):
    sp_size, tp_size = mesh.shape["sp"], mesh.shape["tp"]
    cache_spec = P("dp", "sp", "tp", None)
    row_spec = P("dp", None)
    col_spec = P(None, "tp")
    in_specs = (row_spec, P("dp"), cache_spec, cache_spec, P(None), col_spec, col_spec, col_spec, P("tp", None), P(None), col_spec, col_spec, P("tp", None))
    out_specs = (row_spec, cache_spec, cache_spec)

    def local_step(tokens, positions, cache_k, cache_v, attn_gain, w_q, w_k, w_v, w_o, mlp_gain, w_gate, w_up, w_down):
        rows, depth = tokens.shape
        head_dim = cache_k.shape[3]
        kv_local = cache_k.shape[2]
        q_width, kv_width = w_q.shape[1], w_k.shape[1]
        heads = q_width // head_dim
        width = depth // sp_size
        hidden_width = w_gate.shape[1] // sp_size
        chunks = 7
        cos_table, sin_table = rope_tables(positions, head_dim)
        vmem = pl.BlockSpec(memory_space=pltpu.VMEM)
        hbm = pl.BlockSpec(memory_space=pltpu.HBM)
        dma = pltpu.SemaphoreType.DMA
        in_hbm = functools.partial(pltpu.with_memory_space_constraint, memory_space=pltpu.HBM)
        new_k, new_v, packed = pl.pallas_call(
            functools.partial(attention_kernel, sp_size, chunks),
            out_shape=[pltpu.HBM(cache_k.shape, BF16), pltpu.HBM(cache_v.shape, BF16),
                       pltpu.VMEM((rows, q_width + 128), F32)],
            in_specs=[pl.BlockSpec(memory_space=pltpu.SMEM)] + [vmem] * 4 + [hbm] * 5,
            out_specs=[hbm, hbm, vmem],
            scratch_shapes=[
                pltpu.VMEM((depth, q_width + 2 * kv_width), BF16),
                pltpu.VMEM(cache_k.shape, BF16), pltpu.VMEM(cache_v.shape, BF16),
                pltpu.VMEM((rows, heads, head_dim), F32), pltpu.VMEM((rows, kv_local, head_dim), F32),
                pltpu.VMEM((rows, kv_local, head_dim), F32), pltpu.VMEM((rows, heads, head_dim), F32),
                pltpu.VMEM((rows, heads, 128), F32), pltpu.VMEM((rows, heads, 128), F32),
                dma((chunks, 3)), dma((rows,)), dma((rows,)), dma((rows,)), dma((rows,)),
            ],
            compiler_params=pltpu.CompilerParams(vmem_limit_bytes=40 * 2 ** 20),
            cost_estimate=pl.CostEstimate(flops=10 ** 9, bytes_accessed=48 * 10 ** 6, transcendentals=0),
            name="attention",
        )(positions, tokens, attn_gain[None, :], cos_table, sin_table, *map(in_hbm, (w_q, w_k, w_v, cache_k, cache_v)))

        chunk = pltpu.VMEM((rows, width), F32)
        act = pltpu.VMEM((rows, hidden_width), F32)
        out = pl.pallas_call(
            functools.partial(mlp_kernel, head_dim),
            out_shape=jax.ShapeDtypeStruct((rows, depth), BF16),
            in_specs=[vmem] * 3 + [hbm] * 4,
            out_specs=vmem,
            scratch_shapes=[
                pltpu.VMEM((q_width, width), BF16), pltpu.VMEM((depth, 2 * hidden_width), BF16),
                pltpu.VMEM((w_down.shape[0], width), BF16),
                pltpu.VMEM((sp_size, rows, q_width + 128), F32),
                chunk, pltpu.VMEM((tp_size, rows, width), F32),
                chunk, pltpu.VMEM((sp_size, rows, width), F32),
                act, pltpu.VMEM((sp_size, rows, hidden_width), F32),
                chunk, pltpu.VMEM((tp_size, rows, width), F32),
                chunk, pltpu.VMEM((sp_size, rows, width), F32),
                dma((4,)), dma((6, 3)), dma((6, 3)),
            ],
            compiler_params=pltpu.CompilerParams(vmem_limit_bytes=40 * 2 ** 20, collective_id=0, has_side_effects=True),
            cost_estimate=pl.CostEstimate(flops=10 ** 9, bytes_accessed=21 * 10 ** 6, transcendentals=0),
            name="mlp",
        )(packed, tokens, mlp_gain[None, :], *map(in_hbm, (w_o, w_gate, w_up, w_down)))
        return out, new_k, new_v

    return jax.shard_map(local_step, mesh=mesh, in_specs=in_specs, out_specs=out_specs, check_vma=False)
```

```python
import math
import functools
import jax
import jax.numpy as jnp
from jax import lax
from jax.experimental import pallas as pl
from jax.experimental.pallas import tpu as pltpu
from jax.sharding import PartitionSpec as P

NORM_EPS = 1e-5
ROPE_THETA = 10000.0
MESH = pl.DeviceIdType.MESH
F32 = jnp.float32
BF16 = jnp.bfloat16


def rope_tables(positions, half):
    index = lax.broadcasted_iota(jnp.int32, (positions.shape[0], half), 1).astype(F32)
    angles = positions * jnp.exp(index * (-math.log(ROPE_THETA) / half))
    turns = jnp.floor(angles * (2.0 / math.pi) + 0.5)
    rest = ((angles - turns * 1.5703125) - turns * 4.837512969970703125e-4) - turns * 7.54978995489188216e-8
    square = rest * rest
    sine = rest + rest * square * (-1.0 / 6 + square * (1.0 / 120 + square * (-1.0 / 5040 + square * (1.0 / 362880))))
    cosine = 1.0 + square * (-0.5 + square * (1.0 / 24 + square * (-1.0 / 720 + square * (1.0 / 40320 - square * (1.0 / 3628800)))))
    quadrant = turns.astype(jnp.int32) & 3
    swap = (quadrant & 1) == 1
    cos_value = jnp.where(swap, sine, cosine)
    sin_value = jnp.where(swap, cosine, sine)
    return (jnp.where((quadrant == 1) | (quadrant == 2), -cos_value, cos_value),
            jnp.where(quadrant >= 2, -sin_value, sin_value))


def scaled_norm(wide, gain_ref):
    inv_rms = lax.rsqrt(jnp.mean(wide * wide, axis=-1, keepdims=True) + NORM_EPS)
    gain = gain_ref[...].astype(F32)
    pieces = [(wide[:, i * 128:(i + 1) * 128] * inv_rms * gain[i:i + 1]).astype(BF16) for i in range(wide.shape[1] // 128)]
    return jnp.concatenate(pieces, axis=1)


def attention_kernel(sp_size, chunks, positions, tokens, gain, wq, wk, wv, ck, cv,
                     new_k, new_v, packed_ref,
                     pos_ref, tok_ref, gain_ref, wbuf, kbuf, vbuf, q3, k3, v3, o3, m3, l3,
                     psem, wsem, ksem, vsem, okm, ovm):
    rows, local_slots, kv_local, head_dim = kbuf.shape
    slots = local_slots * sp_size
    depth = tok_ref.shape[1]
    q_width, kv_width = wq.shape[1], wk.shape[1]
    heads = q_width // head_dim
    group = heads // kv_local
    half = head_dim // 2
    step = depth // chunks
    first_slot = lax.axis_index("sp") * local_slots

    small = [pltpu.make_async_copy(tokens, tok_ref, psem.at[0]), pltpu.make_async_copy(gain, gain_ref, psem.at[1]),
             pltpu.make_async_copy(positions, pos_ref, psem.at[2])]
    for copy in small:
        copy.start()
    weight_copies = []
    for c in range(chunks):
        part = pl.ds(c * step, step)
        trio = [
            pltpu.make_async_copy(wq.at[part, :], wbuf.at[part, pl.ds(0, q_width)], wsem.at[c, 0]),
            pltpu.make_async_copy(wk.at[part, :], wbuf.at[part, pl.ds(q_width, kv_width)], wsem.at[c, 1]),
            pltpu.make_async_copy(wv.at[part, :], wbuf.at[part, pl.ds(q_width + kv_width, kv_width)], wsem.at[c, 2]),
        ]
        for copy in trio:
            copy.start()
        weight_copies.append(trio)
    k_in = [pltpu.make_async_copy(ck.at[b], kbuf.at[b], ksem.at[b]) for b in range(rows)]
    v_in = [pltpu.make_async_copy(cv.at[b], vbuf.at[b], vsem.at[b]) for b in range(rows)]
    started = 0

    for copy in small:
        copy.wait()
    normed = scaled_norm(tok_ref[...].astype(F32), gain_ref)
    acc = jnp.zeros((rows, q_width + 2 * kv_width), F32)
    for c in range(chunks):
        for copy in weight_copies[c]:
            copy.wait()
        while started < min(rows, (c + 1) * rows // chunks + 1):
            k_in[started].start()
            v_in[started].start()
            started += 1
        acc = acc + jnp.dot(normed[:, c * step:(c + 1) * step], wbuf[c * step:(c + 1) * step, :], preferred_element_type=F32)

    row = lax.broadcasted_iota(jnp.int32, (rows, half), 0)
    position_rows = jnp.zeros((rows, half), F32)
    for b in range(rows):
        position_rows = jnp.where(row == b, pos_ref[b].astype(F32), position_rows)
    cos_table, sin_table = rope_tables(position_rows, half)
    scale = 1.0 / math.sqrt(head_dim)

    def rotate(start):
        a = acc[:, start:start + half]
        b = acc[:, start + half:start + head_dim]
        return a * cos_table - b * sin_table, b * cos_table + a * sin_table

    for j in range(heads):
        a, b = rotate(j * head_dim)
        q3[:, j, 0:half] = a
        q3[:, j, half:head_dim] = b
    for j in range(kv_local):
        a, b = rotate(q_width + j * head_dim)
        k3[:, j, 0:half] = a
        k3[:, j, half:head_dim] = b
        start = q_width + kv_width + j * head_dim
        v3[:, j, :] = acc[:, start:start + head_dim]

    width = local_slots * kv_local
    column = lax.broadcasted_iota(jnp.int32, (heads, width), 1)
    own_head = lax.rem(column, kv_local) == lax.broadcasted_iota(jnp.int32, (heads, width), 0) // group
    slot_ids = first_slot + column // kv_local
    k_out, v_out = [], []
    for b in range(rows):
        position = pos_ref[b]
        target = lax.rem(position, slots) - first_slot
        k_in[b].wait()
        v_in[b].wait()

        @pl.when((target >= 0) & (target < local_slots))
        def _():
            kbuf[b, target] = k3[b].astype(BF16)
            vbuf[b, target] = v3[b].astype(BF16)

        q_b = q3[b].astype(BF16)
        keys = kbuf[b].reshape(width, head_dim)
        scores = lax.dot_general(q_b, keys, (((1,), (1,)), ((), ())), preferred_element_type=F32) * scale
        limit = jnp.where(position >= slots - 1, slots, position)
        valid = own_head & (slot_ids <= limit)
        scores = jnp.where(valid, scores, -jnp.inf)
        top = jnp.max(scores, axis=1, keepdims=True)
        weights = jnp.where(valid, jnp.exp(scores - top), 0.0)
        k_out.append(pltpu.make_async_copy(kbuf.at[b], new_k.at[b], okm.at[b]))
        v_out.append(pltpu.make_async_copy(vbuf.at[b], new_v.at[b], ovm.at[b]))
        k_out[b].start()
        v_out[b].start()
        o3[b] = jnp.dot(weights.astype(BF16), vbuf[b].reshape(width, head_dim), preferred_element_type=F32)
        m3[b] = jnp.broadcast_to(top, (heads, 128))
        l3[b] = jnp.broadcast_to(jnp.sum(weights, axis=1, keepdims=True), (heads, 128))

    lane = lax.broadcasted_iota(jnp.int32, (rows, 128), 1) // 16
    stats = jnp.zeros((rows, 128), F32)
    for j in range(heads):
        packed_ref[:, j * head_dim:(j + 1) * head_dim] = o3[:, j, :]
        stats = jnp.where(lane == j, m3[:, j, :], stats)
        stats = jnp.where(lane == heads + j, l3[:, j, :], stats)
    packed_ref[:, q_width:q_width + 128] = stats
    for b in range(rows):
        k_out[b].wait()
        v_out[b].wait()


def exchange(axis, source, slots_ref, cols, send_sem, recv_sem):
    me = lax.axis_index(axis)
    size = slots_ref.shape[0]
    copies = []
    for d in range(1, size):
        copy = pltpu.make_async_remote_copy(
            src_ref=source.at[:, cols], dst_ref=slots_ref.at[me, :, cols], send_sem=send_sem.at[d - 1],
            recv_sem=recv_sem.at[d - 1], device_id={axis: lax.rem(me + d, size)}, device_id_type=MESH)
        copy.start()
        copies.append(copy)
    return copies


def finish(copies):
    for copy in copies:
        copy.wait()


def added(slots_ref, cols):
    total = slots_ref[0, :, cols]
    for t in range(1, slots_ref.shape[0]):
        total = total + slots_ref[t, :, cols]
    return total


def mlp_kernel(head_dim, cuts, packed_ref, tokens, gain, wo, wg, wu, wd, out_ref,
               tok_ref, gain_ref, wo_buf, wgu_buf, wd_buf, r1, part2, r2, part3, r3, part4, r4, part5, r5, part6, r6,
               psem, wsem, gsem, dsem, ssem, rsem):
    rows, depth = tokens.shape
    sp_size, tp_size = r1.shape[0], r2.shape[0]
    q_width = wo.shape[0]
    heads = q_width // head_dim
    width = depth // sp_size
    sp = lax.axis_index("sp")
    tp = lax.axis_index("tp")
    start = pl.multiple_of(sp * width, 128)
    my_cols = pl.ds(start, width)
    pieces = [pl.ds(a, b - a) for a, b in zip((0,) + cuts[:-1], cuts)]

    barrier = pltpu.get_barrier_semaphore()
    for axis, me, size in (("sp", sp, sp_size), ("tp", tp, tp_size)):
        for d in range(1, size):
            pl.semaphore_signal(barrier, inc=1, device_id={axis: lax.rem(me + d, size)}, device_id_type=MESH)
    small = [pltpu.make_async_copy(tokens.at[:, my_cols], tok_ref, psem.at[0]), pltpu.make_async_copy(gain, gain_ref, psem.at[1])]
    o_load = pltpu.make_async_copy(wo.at[:, my_cols], wo_buf, wsem)
    gate_loads, down_loads = [], []
    for i, piece in enumerate(pieces):
        cols = pl.ds(start + piece.start, piece.size)
        gate_loads.append([
            pltpu.make_async_copy(wg.at[:, cols], wgu_buf.at[:, pl.ds(2 * piece.start, piece.size)], gsem.at[i, 0]),
            pltpu.make_async_copy(wu.at[:, cols], wgu_buf.at[:, pl.ds(2 * piece.start + piece.size, piece.size)], gsem.at[i, 1])])
        down_loads.append([
            pltpu.make_async_copy(wd.at[pl.ds(s * width + piece.start, piece.size), my_cols],
                                  wd_buf.at[pl.ds(sp_size * piece.start + s * piece.size, piece.size), :], dsem.at[i, s])
            for s in range(sp_size)])
    o_load.start()
    for copy in small:
        copy.start()
    for loads in gate_loads:
        for copy in loads:
            copy.start()
    pl.semaphore_wait(barrier, sp_size + tp_size - 2)

    copies = exchange("sp", packed_ref, r1, pl.ds(0, packed_ref.shape[1]), ssem.at[0, 0], rsem.at[0, 0])
    r1[sp] = packed_ref[...]
    o_load.wait()
    finish(copies)
    for loads in down_loads:
        for copy in loads:
            copy.start()
    stats = [r1[s, :, q_width:q_width + 128] for s in range(sp_size)]
    parts = []
    for j in range(heads):
        tops = [t[:, j * 16:j * 16 + 1] for t in stats]
        best = functools.reduce(jnp.maximum, tops)
        numerator = jnp.zeros((rows, head_dim), F32)
        denominator = jnp.zeros((rows, 1), F32)
        for s in range(sp_size):
            factor = jnp.exp(tops[s] - best)
            numerator = numerator + r1[s, :, j * head_dim:(j + 1) * head_dim] * factor
            denominator = denominator + stats[s][:, (heads + j) * 16:(heads + j) * 16 + 1] * factor
        parts.append((numerator / denominator).astype(BF16))
    attended = jnp.concatenate(parts, axis=1)

    def project(left, weights, source, slots_ref, phase):
        sent = []
        for i, piece in enumerate(pieces):
            source[:, piece] = sum(jnp.dot(l, w[:, piece], preferred_element_type=F32) for l, w in zip(left, weights))
            sent.append(exchange("tp", source, slots_ref, piece, ssem.at[phase, i], rsem.at[phase, i]))
            slots_ref[tp, :, piece] = source[:, piece]
        return sent

    def settle(base, sent, slots_ref, target, target_slots, phase):
        passed = []
        for i, piece in enumerate(pieces):
            finish(sent[i])
            value = (base[:, piece] + added(slots_ref, piece)).astype(BF16).astype(F32)
            target[:, piece] = value
            passed.append(exchange("sp", target, target_slots, piece, ssem.at[phase, i], rsem.at[phase, i]))
            target_slots[sp, :, piece] = value
        return passed

    sent = project([attended], [wo_buf], part2, r2, 1)
    finish(small)
    tok32 = tok_ref[...].astype(F32)
    part6[...] = tok32
    passed = settle(part6, sent, r2, part3, r3, 2)
    for loads in gate_loads:
        finish(loads)
    for copies in passed:
        finish(copies)
    hidden = jnp.concatenate([r3[s] for s in range(sp_size)], axis=1)
    normed = scaled_norm(hidden, gain_ref)

    moved = []
    for i, piece in enumerate(pieces):
        both = jnp.dot(normed, wgu_buf[:, 2 * piece.start:2 * (piece.start + piece.size)], preferred_element_type=F32)
        gate, up = both[:, :piece.size], both[:, piece.size:]
        active = (gate * jax.nn.sigmoid(gate) * up).astype(BF16).astype(F32)
        part4[:, piece] = active
        moved.append(exchange("sp", part4, r4, piece, ssem.at[3, i], rsem.at[3, i]))
        r4[sp, :, piece] = active
    left, weights = [], []
    for i, piece in enumerate(pieces):
        finish(down_loads[i])
    total = None
    for i, piece in enumerate(pieces):
        finish(moved[i])
        left = jnp.concatenate([r4[s, :, piece] for s in range(sp_size)], axis=1).astype(BF16)
        rows_of = wd_buf[sp_size * piece.start:sp_size * (piece.start + piece.size), :]
        if i + 1 < len(pieces):
            product = jnp.dot(left, rows_of, preferred_element_type=F32)
            total = product if total is None else total + product
    part5[...] = total
    sent = []
    for i, piece in enumerate(pieces):
        part5[:, piece] = part5[:, piece] + jnp.dot(left, rows_of[:, piece.start:piece.start + piece.size], preferred_element_type=F32)
        sent.append(exchange("tp", part5, r5, piece, ssem.at[4, i], rsem.at[4, i]))
        r5[tp, :, piece] = part5[:, piece]
    passed = settle(part3, sent, r5, part6, r6, 5)
    for copies in passed:
        finish(copies)
    out_ref[...] = jnp.concatenate([r6[s] for s in range(sp_size)], axis=1).astype(BF16)


def solution(mesh):
    sp_size, tp_size = mesh.shape["sp"], mesh.shape["tp"]
    cache_spec = P("dp", "sp", "tp", None)
    row_spec = P("dp", None)
    col_spec = P(None, "tp")
    in_specs = (row_spec, P("dp"), cache_spec, cache_spec, P(None), col_spec, col_spec, col_spec, P("tp", None), P(None), col_spec, col_spec, P("tp", None))
    out_specs = (row_spec, cache_spec, cache_spec)

    def local_step(tokens, positions, cache_k, cache_v, attn_gain, w_q, w_k, w_v, w_o, mlp_gain, w_gate, w_up, w_down):
        rows, depth = tokens.shape
        head_dim = cache_k.shape[3]
        kv_local = cache_k.shape[2]
        q_width, kv_width = w_q.shape[1], w_k.shape[1]
        heads = q_width // head_dim
        width = depth // sp_size
        hidden_width = w_gate.shape[1] // sp_size
        chunks = 7
        cuts = (512, width)
        vmem = pl.BlockSpec(memory_space=pltpu.VMEM)
        hbm = pl.BlockSpec(memory_space=pltpu.HBM)
        dma = pltpu.SemaphoreType.DMA
        in_hbm = functools.partial(pltpu.with_memory_space_constraint, memory_space=pltpu.HBM)
        new_k, new_v, packed = pl.pallas_call(
            functools.partial(attention_kernel, sp_size, chunks),
            out_shape=[pltpu.HBM(cache_k.shape, BF16), pltpu.HBM(cache_v.shape, BF16),
                       pltpu.VMEM((rows, q_width + 128), F32)],
            in_specs=[hbm] * 8,
            out_specs=[hbm, hbm, vmem],
            scratch_shapes=[
                pltpu.SMEM((rows,), jnp.int32), pltpu.VMEM((rows, depth), BF16), pltpu.VMEM((depth // 128, 128), BF16),
                pltpu.VMEM((depth, q_width + 2 * kv_width), BF16),
                pltpu.VMEM(cache_k.shape, BF16), pltpu.VMEM(cache_v.shape, BF16),
                pltpu.VMEM((rows, heads, head_dim), F32), pltpu.VMEM((rows, kv_local, head_dim), F32),
                pltpu.VMEM((rows, kv_local, head_dim), F32), pltpu.VMEM((rows, heads, head_dim), F32),
                pltpu.VMEM((rows, heads, 128), F32), pltpu.VMEM((rows, heads, 128), F32),
                dma((3,)), dma((chunks, 3)), dma((rows,)), dma((rows,)), dma((rows,)), dma((rows,)),
            ],
            compiler_params=pltpu.CompilerParams(vmem_limit_bytes=40 * 2 ** 20),
            cost_estimate=pl.CostEstimate(flops=10 ** 9, bytes_accessed=48 * 10 ** 6, transcendentals=0),
            name="attention",
        )(*map(in_hbm, (positions, tokens, attn_gain.reshape(depth // 128, 128), w_q, w_k, w_v, cache_k, cache_v)))

        chunk = pltpu.VMEM((rows, width), F32)
        act = pltpu.VMEM((rows, hidden_width), F32)
        out = pl.pallas_call(
            functools.partial(mlp_kernel, head_dim, cuts),
            out_shape=jax.ShapeDtypeStruct((rows, depth), BF16),
            in_specs=[vmem] + [hbm] * 6,
            out_specs=vmem,
            scratch_shapes=[
                pltpu.VMEM((rows, width), BF16), pltpu.VMEM((depth // 128, 128), BF16),
                pltpu.VMEM((q_width, width), BF16), pltpu.VMEM((depth, 2 * hidden_width), BF16),
                pltpu.VMEM((w_down.shape[0], width), BF16),
                pltpu.VMEM((sp_size, rows, q_width + 128), F32),
                chunk, pltpu.VMEM((tp_size, rows, width), F32),
                chunk, pltpu.VMEM((sp_size, rows, width), F32),
                act, pltpu.VMEM((sp_size, rows, hidden_width), F32),
                chunk, pltpu.VMEM((tp_size, rows, width), F32),
                chunk, pltpu.VMEM((sp_size, rows, width), F32),
                dma((2,)), dma, dma((len(cuts), 2)), dma((len(cuts), sp_size)),
                dma((6, len(cuts), 3)), dma((6, len(cuts), 3)),
            ],
            compiler_params=pltpu.CompilerParams(vmem_limit_bytes=40 * 2 ** 20, collective_id=0, has_side_effects=True),
            cost_estimate=pl.CostEstimate(flops=10 ** 9, bytes_accessed=21 * 10 ** 6, transcendentals=0),
            name="mlp",
        )(packed, *map(in_hbm, (tokens, mlp_gain.reshape(depth // 128, 128), w_o, w_gate, w_up, w_down)))
        return out, new_k, new_v

    return jax.shard_map(local_step, mesh=mesh, in_specs=in_specs, out_specs=out_specs, check_vma=False)
```

```python
import math
import functools
import jax
import jax.numpy as jnp
from jax import lax
from jax.experimental import pallas as pl
from jax.experimental.pallas import tpu as pltpu
from jax.sharding import PartitionSpec as P

NORM_EPS = 1e-5
ROPE_THETA = 10000.0
MESH = pl.DeviceIdType.MESH
F32 = jnp.float32
BF16 = jnp.bfloat16


def rope_tables(positions, half):
    index = lax.broadcasted_iota(jnp.int32, (positions.shape[0], half), 1).astype(F32)
    angles = positions * jnp.exp(index * (-math.log(ROPE_THETA) / half))
    turns = jnp.floor(angles * (2.0 / math.pi) + 0.5)
    rest = ((angles - turns * 1.5703125) - turns * 4.837512969970703125e-4) - turns * 7.54978995489188216e-8
    square = rest * rest
    sine = rest + rest * square * (-1.0 / 6 + square * (1.0 / 120 + square * (-1.0 / 5040 + square * (1.0 / 362880))))
    cosine = 1.0 + square * (-0.5 + square * (1.0 / 24 + square * (-1.0 / 720 + square * (1.0 / 40320 - square * (1.0 / 3628800)))))
    quadrant = turns.astype(jnp.int32) & 3
    swap = (quadrant & 1) == 1
    cos_value = jnp.where(swap, sine, cosine)
    sin_value = jnp.where(swap, cosine, sine)
    return (jnp.where((quadrant == 1) | (quadrant == 2), -cos_value, cos_value),
            jnp.where(quadrant >= 2, -sin_value, sin_value))


def scaled_norm(wide, gain_ref):
    inv_rms = lax.rsqrt(jnp.mean(wide * wide, axis=-1, keepdims=True) + NORM_EPS)
    gain = gain_ref[...].astype(F32)
    pieces = [(wide[:, i * 128:(i + 1) * 128] * inv_rms * gain[i:i + 1]).astype(BF16) for i in range(wide.shape[1] // 128)]
    return jnp.concatenate(pieces, axis=1)


def attention_kernel(sp_size, chunks, positions, tokens, gain, wq, wk, wv, ck, cv,
                     kbuf, vbuf, packed_ref,
                     pos_ref, tok_ref, gain_ref, wbuf, q3, k3, v3, o3, m3, l3,
                     psem, wsem, ksem, vsem):
    rows, local_slots, kv_local, head_dim = kbuf.shape
    slots = local_slots * sp_size
    depth = tok_ref.shape[1]
    q_width, kv_width = wq.shape[1], wk.shape[1]
    heads = q_width // head_dim
    group = heads // kv_local
    half = head_dim // 2
    step = depth // chunks
    first_slot = lax.axis_index("sp") * local_slots

    small = [pltpu.make_async_copy(tokens, tok_ref, psem.at[0]), pltpu.make_async_copy(gain, gain_ref, psem.at[1]),
             pltpu.make_async_copy(positions, pos_ref, psem.at[2])]
    for copy in small:
        copy.start()
    weight_copies = []
    for c in range(chunks):
        part = pl.ds(c * step, step)
        trio = [
            pltpu.make_async_copy(wq.at[part, :], wbuf.at[part, pl.ds(0, q_width)], wsem.at[c, 0]),
            pltpu.make_async_copy(wk.at[part, :], wbuf.at[part, pl.ds(q_width, kv_width)], wsem.at[c, 1]),
            pltpu.make_async_copy(wv.at[part, :], wbuf.at[part, pl.ds(q_width + kv_width, kv_width)], wsem.at[c, 2]),
        ]
        for copy in trio:
            copy.start()
        weight_copies.append(trio)
    k_in = [pltpu.make_async_copy(ck.at[b], kbuf.at[b], ksem.at[b]) for b in range(rows)]
    v_in = [pltpu.make_async_copy(cv.at[b], vbuf.at[b], vsem.at[b]) for b in range(rows)]
    started = 0

    for copy in small:
        copy.wait()
    normed = scaled_norm(tok_ref[...].astype(F32), gain_ref)
    acc = jnp.zeros((rows, q_width + 2 * kv_width), F32)
    for c in range(chunks):
        for copy in weight_copies[c]:
            copy.wait()
        while started < min(rows, (c + 1) * rows // chunks + 1):
            k_in[started].start()
            v_in[started].start()
            started += 1
        acc = acc + jnp.dot(normed[:, c * step:(c + 1) * step], wbuf[c * step:(c + 1) * step, :], preferred_element_type=F32)

    row = lax.broadcasted_iota(jnp.int32, (rows, half), 0)
    position_rows = jnp.zeros((rows, half), F32)
    for b in range(rows):
        position_rows = jnp.where(row == b, pos_ref[b].astype(F32), position_rows)
    cos_table, sin_table = rope_tables(position_rows, half)
    scale = 1.0 / math.sqrt(head_dim)

    def rotate(start):
        a = acc[:, start:start + half]
        b = acc[:, start + half:start + head_dim]
        return a * cos_table - b * sin_table, b * cos_table + a * sin_table

    for j in range(heads):
        a, b = rotate(j * head_dim)
        q3[:, j, 0:half] = a
        q3[:, j, half:head_dim] = b
    for j in range(kv_local):
        a, b = rotate(q_width + j * head_dim)
        k3[:, j, 0:half] = a
        k3[:, j, half:head_dim] = b
        start = q_width + kv_width + j * head_dim
        v3[:, j, :] = acc[:, start:start + head_dim]

    width = local_slots * kv_local
    column = lax.broadcasted_iota(jnp.int32, (heads, width), 1)
    own_head = lax.rem(column, kv_local) == lax.broadcasted_iota(jnp.int32, (heads, width), 0) // group
    slot_ids = first_slot + column // kv_local
    for b in range(rows):
        position = pos_ref[b]
        target = lax.rem(position, slots) - first_slot
        k_in[b].wait()
        v_in[b].wait()

        @pl.when((target >= 0) & (target < local_slots))
        def _():
            kbuf[b, target] = k3[b].astype(BF16)
            vbuf[b, target] = v3[b].astype(BF16)

        q_b = q3[b].astype(BF16)
        keys = kbuf[b].reshape(width, head_dim)
        scores = lax.dot_general(q_b, keys, (((1,), (1,)), ((), ())), preferred_element_type=F32) * scale
        limit = jnp.where(position >= slots - 1, slots, position)
        valid = own_head & (slot_ids <= limit)
        scores = jnp.where(valid, scores, -jnp.inf)
        top = jnp.max(scores, axis=1, keepdims=True)
        weights = jnp.where(valid, jnp.exp(scores - top), 0.0)
        o3[b] = jnp.dot(weights.astype(BF16), vbuf[b].reshape(width, head_dim), preferred_element_type=F32)
        m3[b] = jnp.broadcast_to(top, (heads, 128))
        l3[b] = jnp.broadcast_to(jnp.sum(weights, axis=1, keepdims=True), (heads, 128))

    lane = lax.broadcasted_iota(jnp.int32, (rows, 128), 1) // 16
    stats = jnp.zeros((rows, 128), F32)
    for j in range(heads):
        packed_ref[:, j * head_dim:(j + 1) * head_dim] = o3[:, j, :]
        stats = jnp.where(lane == j, m3[:, j, :], stats)
        stats = jnp.where(lane == heads + j, l3[:, j, :], stats)
    packed_ref[:, q_width:q_width + 128] = stats


def write_kernel(kbuf, vbuf, wo, new_k, new_v, wo_buf, ksem, vsem, wsem):
    rows = kbuf.shape[0]
    width = wo_buf.shape[1]
    cols = pl.ds(pl.multiple_of(lax.axis_index("sp") * width, 128), width)
    copies = [pltpu.make_async_copy(wo.at[:, cols], wo_buf, wsem)]
    for b in range(rows):
        copies.append(pltpu.make_async_copy(kbuf.at[b], new_k.at[b], ksem.at[b]))
        copies.append(pltpu.make_async_copy(vbuf.at[b], new_v.at[b], vsem.at[b]))
    for copy in copies:
        copy.start()
    for copy in copies:
        copy.wait()


def exchange(axis, source, slots_ref, cols, send_sem, recv_sem):
    me = lax.axis_index(axis)
    size = slots_ref.shape[0]
    copies = []
    for d in range(1, size):
        copy = pltpu.make_async_remote_copy(
            src_ref=source.at[:, cols], dst_ref=slots_ref.at[me, :, cols], send_sem=send_sem.at[d - 1],
            recv_sem=recv_sem.at[d - 1], device_id={axis: lax.rem(me + d, size)}, device_id_type=MESH)
        copy.start()
        copies.append(copy)
    return copies


def finish(copies):
    for copy in copies:
        copy.wait()


def added(slots_ref, cols):
    total = slots_ref[0, :, cols]
    for t in range(1, slots_ref.shape[0]):
        total = total + slots_ref[t, :, cols]
    return total


def mlp_kernel(head_dim, cuts, sp_size, *refs):
    r1 = refs[:sp_size]
    (wo_buf, tokens, gain, wg, wu, wd, out_ref,
               tok_ref, gain_ref, wgu_buf, wd_buf, part2, r2, part3, r3, part4, r4, part5, r5, part6, r6,
               psem, gsem, dsem, ssem, rsem) = refs[sp_size:]
    rows, depth = tokens.shape
    tp_size = r2.shape[0]
    q_width = wo_buf.shape[0]
    heads = q_width // head_dim
    width = depth // sp_size
    sp = lax.axis_index("sp")
    tp = lax.axis_index("tp")
    start = pl.multiple_of(sp * width, 128)
    my_cols = pl.ds(start, width)
    pieces = [pl.ds(a, b - a) for a, b in zip((0,) + cuts[:-1], cuts)]

    barrier = pltpu.get_barrier_semaphore()
    for axis, me, size in (("sp", sp, sp_size), ("tp", tp, tp_size)):
        for d in range(1, size):
            pl.semaphore_signal(barrier, inc=1, device_id={axis: lax.rem(me + d, size)}, device_id_type=MESH)
    small = [pltpu.make_async_copy(tokens.at[:, my_cols], tok_ref, psem.at[0]), pltpu.make_async_copy(gain, gain_ref, psem.at[1])]
    gate_loads, down_loads = [], []
    for i, piece in enumerate(pieces):
        cols = pl.ds(start + piece.start, piece.size)
        gate_loads.append([
            pltpu.make_async_copy(wg.at[:, cols], wgu_buf.at[:, pl.ds(2 * piece.start, piece.size)], gsem.at[i, 0]),
            pltpu.make_async_copy(wu.at[:, cols], wgu_buf.at[:, pl.ds(2 * piece.start + piece.size, piece.size)], gsem.at[i, 1])])
        down_loads.append([
            pltpu.make_async_copy(wd.at[pl.ds(s * width + piece.start, piece.size), my_cols],
                                  wd_buf.at[pl.ds(sp_size * piece.start + s * piece.size, piece.size), :], dsem.at[i, s])
            for s in range(sp_size)])
    for copy in small:
        copy.start()
    for loads in gate_loads:
        for copy in loads:
            copy.start()
    for loads in down_loads:
        for copy in loads:
            copy.start()
    stats = [r1[s][:, q_width:q_width + 128] for s in range(sp_size)]
    parts = []
    for j in range(heads):
        tops = [t[:, j * 16:j * 16 + 1] for t in stats]
        best = functools.reduce(jnp.maximum, tops)
        numerator = jnp.zeros((rows, head_dim), F32)
        denominator = jnp.zeros((rows, 1), F32)
        for s in range(sp_size):
            factor = jnp.exp(tops[s] - best)
            numerator = numerator + r1[s][:, j * head_dim:(j + 1) * head_dim] * factor
            denominator = denominator + stats[s][:, (heads + j) * 16:(heads + j) * 16 + 1] * factor
        parts.append((numerator / denominator).astype(BF16))
    attended = jnp.concatenate(parts, axis=1)

    def project(left, weights, source, slots_ref, phase):
        sent = []
        for i, piece in enumerate(pieces):
            source[:, piece] = sum(jnp.dot(l, w[:, piece], preferred_element_type=F32) for l, w in zip(left, weights))
            if i == 0:
                pl.semaphore_wait(barrier, sp_size + tp_size - 2)
            sent.append(exchange("tp", source, slots_ref, piece, ssem.at[phase, i], rsem.at[phase, i]))
            slots_ref[tp, :, piece] = source[:, piece]
        return sent

    def settle(base, sent, slots_ref, target, target_slots, phase):
        passed = []
        for i, piece in enumerate(pieces):
            finish(sent[i])
            value = (base[:, piece] + added(slots_ref, piece)).astype(BF16).astype(F32)
            target[:, piece] = value
            passed.append(exchange("sp", target, target_slots, piece, ssem.at[phase, i], rsem.at[phase, i]))
            target_slots[sp, :, piece] = value
        return passed

    sent = project([attended], [wo_buf], part2, r2, 0)
    finish(small)
    tok32 = tok_ref[...].astype(F32)
    part6[...] = tok32
    passed = settle(part6, sent, r2, part3, r3, 1)
    for loads in gate_loads:
        finish(loads)
    for copies in passed:
        finish(copies)
    hidden = jnp.concatenate([r3[s] for s in range(sp_size)], axis=1)
    normed = scaled_norm(hidden, gain_ref)

    moved = []
    for i, piece in enumerate(pieces):
        both = jnp.dot(normed, wgu_buf[:, 2 * piece.start:2 * (piece.start + piece.size)], preferred_element_type=F32)
        gate, up = both[:, :piece.size], both[:, piece.size:]
        active = (gate * jax.nn.sigmoid(gate) * up).astype(BF16).astype(F32)
        part4[:, piece] = active
        moved.append(exchange("sp", part4, r4, piece, ssem.at[2, i], rsem.at[2, i]))
        r4[sp, :, piece] = active
    left, weights = [], []
    for i, piece in enumerate(pieces):
        finish(down_loads[i])
    total = None
    for i, piece in enumerate(pieces):
        finish(moved[i])
        left = jnp.concatenate([r4[s, :, piece] for s in range(sp_size)], axis=1).astype(BF16)
        rows_of = wd_buf[sp_size * piece.start:sp_size * (piece.start + piece.size), :]
        if i + 1 < len(pieces):
            product = jnp.dot(left, rows_of, preferred_element_type=F32)
            total = product if total is None else total + product
    part5[...] = total
    sent = []
    for i, piece in enumerate(pieces):
        part5[:, piece] = part5[:, piece] + jnp.dot(left, rows_of[:, piece.start:piece.start + piece.size], preferred_element_type=F32)
        sent.append(exchange("tp", part5, r5, piece, ssem.at[3, i], rsem.at[3, i]))
        r5[tp, :, piece] = part5[:, piece]
    passed = settle(part3, sent, r5, part6, r6, 4)
    for copies in passed:
        finish(copies)
    out_ref[...] = jnp.concatenate([r6[s] for s in range(sp_size)], axis=1).astype(BF16)


def solution(mesh):
    sp_size, tp_size = mesh.shape["sp"], mesh.shape["tp"]
    cache_spec = P("dp", "sp", "tp", None)
    row_spec = P("dp", None)
    col_spec = P(None, "tp")
    in_specs = (row_spec, P("dp"), cache_spec, cache_spec, P(None), col_spec, col_spec, col_spec, P("tp", None), P(None), col_spec, col_spec, P("tp", None))
    out_specs = (row_spec, cache_spec, cache_spec)

    def local_step(tokens, positions, cache_k, cache_v, attn_gain, w_q, w_k, w_v, w_o, mlp_gain, w_gate, w_up, w_down):
        rows, depth = tokens.shape
        head_dim = cache_k.shape[3]
        kv_local = cache_k.shape[2]
        q_width, kv_width = w_q.shape[1], w_k.shape[1]
        heads = q_width // head_dim
        width = depth // sp_size
        hidden_width = w_gate.shape[1] // sp_size
        chunks = 7
        cuts = (512, width)
        vmem = pl.BlockSpec(memory_space=pltpu.VMEM)
        hbm = pl.BlockSpec(memory_space=pltpu.HBM)
        dma = pltpu.SemaphoreType.DMA
        in_hbm = functools.partial(pltpu.with_memory_space_constraint, memory_space=pltpu.HBM)
        k_here, v_here, packed = pl.pallas_call(
            functools.partial(attention_kernel, sp_size, chunks),
            out_shape=[pltpu.VMEM(cache_k.shape, BF16), pltpu.VMEM(cache_v.shape, BF16),
                       pltpu.VMEM((rows, q_width + 128), F32)],
            in_specs=[hbm] * 8,
            out_specs=[vmem] * 3,
            scratch_shapes=[
                pltpu.SMEM((rows,), jnp.int32), pltpu.VMEM((rows, depth), BF16), pltpu.VMEM((depth // 128, 128), BF16),
                pltpu.VMEM((depth, q_width + 2 * kv_width), BF16),
                pltpu.VMEM((rows, heads, head_dim), F32), pltpu.VMEM((rows, kv_local, head_dim), F32),
                pltpu.VMEM((rows, kv_local, head_dim), F32), pltpu.VMEM((rows, heads, head_dim), F32),
                pltpu.VMEM((rows, heads, 128), F32), pltpu.VMEM((rows, heads, 128), F32),
                dma((3,)), dma((chunks, 3)), dma((rows,)), dma((rows,)),
            ],
            compiler_params=pltpu.CompilerParams(vmem_limit_bytes=20 * 2 ** 20),
            cost_estimate=pl.CostEstimate(flops=10 ** 9, bytes_accessed=48 * 10 ** 6, transcendentals=0),
            name="attention",
        )(*map(in_hbm, (positions, tokens, attn_gain.reshape(depth // 128, 128), w_q, w_k, w_v, cache_k, cache_v)))

        parts = [packed]
        for d in range(1, sp_size):
            parts.append(lax.ppermute(packed, "sp", [(i, (i + d) % sp_size) for i in range(sp_size)]))
        in_vmem = functools.partial(pltpu.with_memory_space_constraint, memory_space=pltpu.VMEM)
        new_k, new_v, wo_here = pl.pallas_call(
            write_kernel,
            out_shape=[pltpu.HBM(cache_k.shape, BF16), pltpu.HBM(cache_v.shape, BF16), pltpu.VMEM((q_width, width), BF16)],
            in_specs=[vmem, vmem, hbm],
            out_specs=[hbm, hbm, vmem],
            scratch_shapes=[dma((rows,)), dma((rows,)), dma],
            compiler_params=pltpu.CompilerParams(vmem_limit_bytes=4 * 2 ** 20),
            cost_estimate=pl.CostEstimate(flops=5 * 10 ** 9, bytes_accessed=18 * 10 ** 6, transcendentals=0),
            name="write",
        )(in_vmem(k_here), in_vmem(v_here), in_hbm(w_o))

        chunk = pltpu.VMEM((rows, width), F32)
        act = pltpu.VMEM((rows, hidden_width), F32)
        out = pl.pallas_call(
            functools.partial(mlp_kernel, head_dim, cuts, sp_size),
            out_shape=jax.ShapeDtypeStruct((rows, depth), BF16),
            in_specs=[vmem] * (sp_size + 1) + [hbm] * 5,
            out_specs=vmem,
            scratch_shapes=[
                pltpu.VMEM((rows, width), BF16), pltpu.VMEM((depth // 128, 128), BF16),
                pltpu.VMEM((depth, 2 * hidden_width), BF16), pltpu.VMEM((w_down.shape[0], width), BF16),
                chunk, pltpu.VMEM((tp_size, rows, width), F32),
                chunk, pltpu.VMEM((sp_size, rows, width), F32),
                act, pltpu.VMEM((sp_size, rows, hidden_width), F32),
                chunk, pltpu.VMEM((tp_size, rows, width), F32),
                chunk, pltpu.VMEM((sp_size, rows, width), F32),
                dma((2,)), dma((len(cuts), 2)), dma((len(cuts), sp_size)),
                dma((5, len(cuts), 3)), dma((5, len(cuts), 3)),
            ],
            compiler_params=pltpu.CompilerParams(vmem_limit_bytes=26 * 2 ** 20, collective_id=0, has_side_effects=True),
            cost_estimate=pl.CostEstimate(flops=10 ** 9, bytes_accessed=21 * 10 ** 6, transcendentals=0),
            name="mlp",
        )(*map(in_vmem, parts + [wo_here]), *map(in_hbm, (tokens, mlp_gain.reshape(depth // 128, 128), w_gate, w_up, w_down)))
        return out, new_k, new_v

    return jax.shard_map(local_step, mesh=mesh, in_specs=in_specs, out_specs=out_specs, check_vma=False)
```

```python
import math
import functools
import jax
import jax.numpy as jnp
from jax import lax
from jax.experimental import pallas as pl
from jax.experimental.pallas import tpu as pltpu
from jax.sharding import PartitionSpec as P

NORM_EPS = 1e-5
ROPE_THETA = 10000.0
MESH = pl.DeviceIdType.MESH
F32 = jnp.float32
BF16 = jnp.bfloat16


def rope_tables(positions, half):
    index = lax.broadcasted_iota(jnp.int32, (positions.shape[0], half), 1).astype(F32)
    angles = positions * jnp.exp(index * (-math.log(ROPE_THETA) / half))
    turns = jnp.floor(angles * (2.0 / math.pi) + 0.5)
    rest = ((angles - turns * 1.5703125) - turns * 4.837512969970703125e-4) - turns * 7.54978995489188216e-8
    square = rest * rest
    sine = rest + rest * square * (-1.0 / 6 + square * (1.0 / 120 + square * (-1.0 / 5040 + square * (1.0 / 362880))))
    cosine = 1.0 + square * (-0.5 + square * (1.0 / 24 + square * (-1.0 / 720 + square * (1.0 / 40320 - square * (1.0 / 3628800)))))
    quadrant = turns.astype(jnp.int32) & 3
    swap = (quadrant & 1) == 1
    cos_value = jnp.where(swap, sine, cosine)
    sin_value = jnp.where(swap, cosine, sine)
    return (jnp.where((quadrant == 1) | (quadrant == 2), -cos_value, cos_value),
            jnp.where(quadrant >= 2, -sin_value, sin_value))


def scaled_norm(wide, gain_ref):
    inv_rms = lax.rsqrt(jnp.mean(wide * wide, axis=-1, keepdims=True) + NORM_EPS)
    gain = gain_ref[...].astype(F32)
    pieces = [(wide[:, i * 128:(i + 1) * 128] * inv_rms * gain[i:i + 1]).astype(BF16) for i in range(wide.shape[1] // 128)]
    return jnp.concatenate(pieces, axis=1)


def exchange(axis, source, slots_ref, send_sem, recv_sem):
    me = lax.axis_index(axis)
    size = slots_ref[0].shape[0]
    dst, cols = slots_ref
    copies = []
    for i in range(size - 1):
        down, up = size - 1 - i, i
        low = jnp.where(down > me, down, down - 1)
        high = jnp.where(up < me, up, up + 1)
        peer = jnp.where(me < size // 2, low, high)
        copies.append((
            pltpu.make_async_remote_copy(
                src_ref=source, dst_ref=dst.at[(me,) + cols], send_sem=send_sem.at[peer], recv_sem=recv_sem.at[me],
                device_id={axis: peer}, device_id_type=MESH),
            pltpu.make_async_remote_copy(
                src_ref=source, dst_ref=dst.at[(peer,) + cols], send_sem=send_sem.at[peer], recv_sem=recv_sem.at[peer],
                device_id={axis: peer}, device_id_type=MESH)))
        copies[-1][0].start()
    return copies


def finish(copies):
    for sent, arriving in copies:
        arriving.wait_recv()
    for sent, arriving in copies:
        sent.wait_send()


def added(slots_ref, cols):
    total = slots_ref[0, :, cols]
    for t in range(1, slots_ref.shape[0]):
        total = total + slots_ref[t, :, cols]
    return total


def layer_kernel(sp_size, tp_size, cuts, positions, tokens, attn_gain, mlp_gain, wq, wk, wv, ck, cv, wo, wg, wu, wd,
                 kbuf, vbuf, k_row, v_row, out_ref,
                 pos_ref, tok_ref, tok_cols, ag_ref, mg_ref, wqkv_buf, wo_buf, wgu_buf, wd_buf,
                 part0, r0, q3, k3, v3, o3, m3, l3, part1, r1, att, part2, r2, part3, r3, part4, r4, part5, r5, part6, r6,
                 psem, wsem, ksem, vsem, osem, gsem, dsem, ssem0, rsem0, ssem1, rsem1, ssem, rsem):
    rows, depth = tokens.shape
    _, local_slots, kv_local, head_dim = ck.shape
    slots = local_slots * sp_size
    q_width, kv_width = wq.shape[1], wk.shape[1]
    heads = q_width // head_dim
    group = heads // kv_local
    half = head_dim // 2
    width = depth // sp_size
    q_cols, kv_cols = q_width // sp_size, kv_width // sp_size
    flat = local_slots * kv_local
    sp, tp = lax.axis_index("sp"), lax.axis_index("tp")
    first_slot = sp * local_slots
    start = pl.multiple_of(sp * width, 128)
    my_cols = pl.ds(start, width)
    pieces = [pl.ds(a, b - a) for a, b in zip((0,) + cuts[:-1], cuts)]

    barrier = pltpu.get_barrier_semaphore()
    for axis, me, size in (("sp", sp, sp_size), ("tp", tp, tp_size)):
        for d in range(1, size):
            pl.semaphore_signal(barrier, inc=1, device_id={axis: lax.rem(me + d, size)}, device_id_type=MESH)

    small = [pltpu.make_async_copy(tokens, tok_ref, psem.at[0]), pltpu.make_async_copy(attn_gain, ag_ref, psem.at[1]),
             pltpu.make_async_copy(positions, pos_ref, psem.at[2]), pltpu.make_async_copy(mlp_gain, mg_ref, psem.at[3]),
             pltpu.make_async_copy(tokens.at[:, my_cols], tok_cols, psem.at[4])]
    q_part = pl.ds(pl.multiple_of(sp * q_cols, 128), q_cols)
    kv_part = pl.ds(pl.multiple_of(sp * kv_cols, 128), kv_cols)
    qkv_loads = [pltpu.make_async_copy(wq.at[:, q_part], wqkv_buf.at[:, pl.ds(0, q_cols)], wsem.at[0]),
                 pltpu.make_async_copy(wk.at[:, kv_part], wqkv_buf.at[:, pl.ds(q_cols, kv_cols)], wsem.at[1]),
                 pltpu.make_async_copy(wv.at[:, kv_part], wqkv_buf.at[:, pl.ds(q_cols + kv_cols, kv_cols)], wsem.at[2])]
    k_flat, v_flat = ck.reshape(rows, flat, head_dim), cv.reshape(rows, flat, head_dim)
    k_in = [pltpu.make_async_copy(k_flat.at[b], kbuf.at[b], ksem.at[b]) for b in range(rows)]
    v_in = [pltpu.make_async_copy(v_flat.at[b], vbuf.at[b], vsem.at[b]) for b in range(rows)]
    o_load = pltpu.make_async_copy(wo.at[:, my_cols], wo_buf, osem)
    gate_loads, down_loads = [], []
    for i, piece in enumerate(pieces):
        cols = pl.ds(start + piece.start, piece.size)
        gate_loads.append([
            pltpu.make_async_copy(wg.at[:, cols], wgu_buf.at[:, pl.ds(2 * piece.start, piece.size)], gsem.at[i, 0]),
            pltpu.make_async_copy(wu.at[:, cols], wgu_buf.at[:, pl.ds(2 * piece.start + piece.size, piece.size)], gsem.at[i, 1])])
        down_loads.append([
            pltpu.make_async_copy(wd.at[pl.ds(s * width + piece.start, piece.size), my_cols],
                                  wd_buf.at[pl.ds(sp_size * piece.start + s * piece.size, piece.size), :], dsem.at[i, s])
            for s in range(sp_size)])
    for copy in small + qkv_loads:
        copy.start()
    for b in range(rows):
        k_in[b].start()
        v_in[b].start()
    o_load.start()
    for loads in gate_loads + down_loads:
        for copy in loads:
            copy.start()

    for copy in small:
        copy.wait()
    normed = scaled_norm(tok_ref[...].astype(F32), ag_ref)
    for copy in qkv_loads:
        copy.wait()
    mine = jnp.dot(normed, wqkv_buf[...], preferred_element_type=F32)
    part0[...] = mine
    pl.semaphore_wait(barrier, sp_size + tp_size - 2)
    moved = exchange("sp", part0, (r0, ()), ssem0, rsem0)
    r0[sp] = mine

    row = lax.broadcasted_iota(jnp.int32, (rows, half), 0)
    position_rows = jnp.zeros((rows, half), F32)
    for b in range(rows):
        position_rows = jnp.where(row == b, pos_ref[b].astype(F32), position_rows)
    cos_table, sin_table = rope_tables(position_rows, half)
    scale = 1.0 / math.sqrt(head_dim)
    column = lax.broadcasted_iota(jnp.int32, (heads, flat), 1)
    own_head = lax.rem(column, kv_local) == lax.broadcasted_iota(jnp.int32, (heads, flat), 0) // group
    slot_ids = first_slot + column // kv_local
    finish(moved)

    def rotate(a, b):
        return a * cos_table - b * sin_table, b * cos_table + a * sin_table

    def gathered(offset, size, index):
        s, at = index * half // size, index * half % size
        return r0[s, :, offset + at:offset + at + half]

    for j in range(heads):
        a, b = rotate(gathered(0, q_cols, 2 * j), gathered(0, q_cols, 2 * j + 1))
        q3[:, j, 0:half] = a
        q3[:, j, half:head_dim] = b
    for j in range(kv_local):
        a, b = rotate(gathered(q_cols, kv_cols, 2 * j), gathered(q_cols, kv_cols, 2 * j + 1))
        k3[:, j, 0:half] = a
        k3[:, j, half:head_dim] = b
        v3[:, j, 0:half] = gathered(q_cols + kv_cols, kv_cols, 2 * j)
        v3[:, j, half:head_dim] = gathered(q_cols + kv_cols, kv_cols, 2 * j + 1)
    k_row[...] = k3[...].astype(BF16)
    v_row[...] = v3[...].astype(BF16)

    def per_query(pair):
        return jnp.concatenate([jnp.broadcast_to(pair[h:h + 1], (group, head_dim)) for h in range(kv_local)], axis=0)

    sends = []
    side = part1.shape[1]
    lane = lax.broadcasted_iota(jnp.int32, (side, 128), 1) // 16
    for b in range(rows):
        position = pos_ref[b]
        target = lax.rem(position, slots)
        limit = jnp.where(position >= slots - 1, slots, position)
        k_in[b].wait()
        v_in[b].wait()
        q_b = q3[b].astype(BF16)
        new_key = per_query(k3[b].astype(BF16).astype(F32))
        new_value = per_query(v3[b].astype(BF16).astype(F32))
        new_score = jnp.sum(q_b.astype(F32) * new_key, axis=1, keepdims=True) * scale
        scores = lax.dot_general(q_b, kbuf[b], (((1,), (1,)), ((), ())), preferred_element_type=F32) * scale
        fresh = slot_ids == target
        valid = own_head & (slot_ids <= limit)
        scores = jnp.where(valid, jnp.where(fresh, new_score, scores), -jnp.inf)
        top = jnp.max(scores, axis=1, keepdims=True)
        weights = jnp.where(valid, jnp.exp(scores - top), 0.0)
        stored = jnp.where(fresh, 0.0, weights)
        new_weight = jnp.sum(jnp.where(fresh, weights, 0.0), axis=1, keepdims=True)
        o3[b] = (jnp.dot(stored.astype(BF16), vbuf[b], preferred_element_type=F32)
                 + new_weight.astype(BF16).astype(F32) * new_value)
        m3[b] = jnp.broadcast_to(top, (heads, 128))
        l3[b] = jnp.broadcast_to(jnp.sum(weights, axis=1, keepdims=True), (heads, 128))
        if (b + 1) % side == 0:
            g = b // side
            members = pl.ds(g * side, side)
            stats = jnp.zeros((side, 128), F32)
            for j in range(heads):
                part1[g, :, j * head_dim:(j + 1) * head_dim] = o3[members, j, :]
                stats = jnp.where(lane == j, m3[members, j, :], stats)
                stats = jnp.where(lane == heads + j, l3[members, j, :], stats)
            part1[g, :, q_width:q_width + 128] = stats
            sends.append(exchange("sp", part1.at[g], (r1, (g,)), ssem1.at[g], rsem1.at[g]))
            r1[sp, g] = part1[g]

    for g, copies in enumerate(sends):
        finish(copies)
        stats = [r1[s, g, :, q_width:q_width + 128] for s in range(sp_size)]
        for j in range(heads):
            tops = [t[:, j * 16:j * 16 + 1] for t in stats]
            best = functools.reduce(jnp.maximum, tops)
            numerator = jnp.zeros((side, head_dim), F32)
            denominator = jnp.zeros((side, 1), F32)
            for s in range(sp_size):
                factor = jnp.exp(tops[s] - best)
                numerator = numerator + r1[s, g, :, j * head_dim:(j + 1) * head_dim] * factor
                denominator = denominator + stats[s][:, (heads + j) * 16:(heads + j) * 16 + 1] * factor
            att[g * side:(g + 1) * side, j * head_dim:(j + 1) * head_dim] = numerator / denominator
    attended = att[...].astype(BF16)

    def pass_on(axis, me, source, slots_ref, phase, i):
        piece = pieces[i]
        copies = exchange(axis, source.at[:, piece], (slots_ref, (slice(None), piece)), ssem.at[phase, i], rsem.at[phase, i])
        slots_ref[me, :, piece] = source[:, piece]
        return copies

    def settle(base, sent, slots_ref, target, target_slots, phase):
        passed = []
        for i, piece in enumerate(pieces):
            finish(sent[i])
            target[:, piece] = (base[:, piece] + added(slots_ref, piece)).astype(BF16).astype(F32)
            passed.append(pass_on("sp", sp, target, target_slots, phase, i))
        return passed

    o_load.wait()
    sent = []
    for i, piece in enumerate(pieces):
        part2[:, piece] = jnp.dot(attended, wo_buf[:, piece], preferred_element_type=F32)
        sent.append(pass_on("tp", tp, part2, r2, 0, i))
    part6[...] = tok_cols[...].astype(F32)
    passed = settle(part6, sent, r2, part3, r3, 1)
    for loads in gate_loads + down_loads:
        for copy in loads:
            copy.wait()
    for copies in passed:
        finish(copies)
    normed = scaled_norm(jnp.concatenate([r3[s] for s in range(sp_size)], axis=1), mg_ref)

    moved = []
    for i, piece in enumerate(pieces):
        both = jnp.dot(normed, wgu_buf[:, 2 * piece.start:2 * (piece.start + piece.size)], preferred_element_type=F32)
        gate, up = both[:, :piece.size], both[:, piece.size:]
        part4[:, piece] = (gate * jax.nn.sigmoid(gate) * up).astype(BF16).astype(F32)
        moved.append(pass_on("sp", sp, part4, r4, 2, i))
    total = None
    for i, piece in enumerate(pieces):
        finish(moved[i])
        left = jnp.concatenate([r4[s, :, piece] for s in range(sp_size)], axis=1).astype(BF16)
        down = pl.ds(sp_size * piece.start, sp_size * piece.size)
        if i + 1 < len(pieces):
            product = jnp.dot(left, wd_buf[down, :], preferred_element_type=F32)
            total = product if total is None else total + product
    part5[...] = total
    sent = []
    for i, piece in enumerate(pieces):
        part5[:, piece] = part5[:, piece] + jnp.dot(left, wd_buf[down, piece], preferred_element_type=F32)
        sent.append(pass_on("tp", tp, part5, r5, 3, i))
    passed = settle(part3, sent, r5, part6, r6, 4)
    for copies in passed:
        finish(copies)
    out_ref[...] = jnp.concatenate([r6[s] for s in range(sp_size)], axis=1).astype(BF16)


def write_kernel(sp_size, pos_ref, k_in, v_in, k_row, v_row, out_in, new_k, new_v, out_ref, kbuf, vbuf, ksem, vsem, osem):
    rows, local_slots, kv_local, head_dim = new_k.shape
    flat = local_slots * kv_local
    tile = 16
    first_slot = lax.axis_index("sp") * local_slots
    copies = [pltpu.make_async_copy(out_in, out_ref, osem)]
    k_flat, v_flat = new_k.reshape(rows, flat, head_dim), new_v.reshape(rows, flat, head_dim)
    for b in range(rows):
        target = lax.rem(pos_ref[b], local_slots * sp_size) - first_slot

        @pl.when((target >= 0) & (target < local_slots))
        def _():
            base = pl.multiple_of((target * kv_local) // tile * tile, tile)
            at = target * kv_local - base
            row = lax.broadcasted_iota(jnp.int32, (tile, head_dim), 0)
            for buf, fresh in ((kbuf, k_row), (vbuf, v_row)):
                block = buf[b, pl.ds(base, tile), :].astype(F32)
                pair = fresh[b].astype(F32)
                for h in range(kv_local):
                    block = jnp.where(row == at + h, pair[h:h + 1], block)
                buf[b, pl.ds(base, tile), :] = block.astype(BF16)

    for b in range(rows):
        copies.append(pltpu.make_async_copy(kbuf.at[b], k_flat.at[b], ksem.at[b]))
        copies.append(pltpu.make_async_copy(vbuf.at[b], v_flat.at[b], vsem.at[b]))
    for copy in copies:
        copy.start()
    for copy in copies:
        copy.wait()


def solution(mesh):
    sp_size, tp_size = mesh.shape["sp"], mesh.shape["tp"]
    cache_spec = P("dp", "sp", "tp", None)
    row_spec = P("dp", None)
    col_spec = P(None, "tp")
    in_specs = (row_spec, P("dp"), cache_spec, cache_spec, P(None), col_spec, col_spec, col_spec, P("tp", None), P(None), col_spec, col_spec, P("tp", None))
    out_specs = (row_spec, cache_spec, cache_spec)

    def local_step(tokens, positions, cache_k, cache_v, attn_gain, w_q, w_k, w_v, w_o, mlp_gain, w_gate, w_up, w_down):
        rows, depth = tokens.shape
        _, local_slots, kv_local, head_dim = cache_k.shape
        q_width, kv_width = w_q.shape[1], w_k.shape[1]
        heads = q_width // head_dim
        width = depth // sp_size
        cuts = (512, width)
        groups = 2
        flat_shape = (rows, local_slots * kv_local, head_dim)
        vmem = pl.BlockSpec(memory_space=pltpu.VMEM)
        hbm = pl.BlockSpec(memory_space=pltpu.HBM)
        dma = pltpu.SemaphoreType.DMA
        in_hbm = functools.partial(pltpu.with_memory_space_constraint, memory_space=pltpu.HBM)
        in_vmem = functools.partial(pltpu.with_memory_space_constraint, memory_space=pltpu.VMEM)
        f32 = lambda *shape: pltpu.VMEM(shape, F32)
        bf16 = lambda *shape: pltpu.VMEM(shape, BF16)
        qkv_cols = (q_width + 2 * kv_width) // sp_size
        packed = (groups, rows // groups, q_width + 128)
        k_here, v_here, k_row, v_row, out_here = pl.pallas_call(
            functools.partial(layer_kernel, sp_size, tp_size, cuts),
            out_shape=[bf16(*flat_shape), bf16(*flat_shape), bf16(rows, kv_local, head_dim), bf16(rows, kv_local, head_dim), bf16(rows, depth)],
            in_specs=[hbm] * 13,
            out_specs=[vmem] * 5,
            scratch_shapes=[
                pltpu.SMEM((rows,), jnp.int32), bf16(rows, depth), bf16(rows, width), bf16(depth // 128, 128), bf16(depth // 128, 128),
                bf16(depth, qkv_cols), bf16(q_width, width), bf16(depth, 2 * width), bf16(w_down.shape[0], width),
                f32(rows, qkv_cols), f32(sp_size, rows, qkv_cols),
                f32(rows, heads, head_dim), f32(rows, kv_local, head_dim), f32(rows, kv_local, head_dim),
                f32(rows, heads, head_dim), f32(rows, heads, 128), f32(rows, heads, 128),
                f32(*packed), f32(sp_size, *packed), f32(rows, q_width),
                f32(rows, width), f32(tp_size, rows, width), f32(rows, width), f32(sp_size, rows, width),
                f32(rows, width), f32(sp_size, rows, width), f32(rows, width), f32(tp_size, rows, width),
                f32(rows, width), f32(sp_size, rows, width),
                dma((5,)), dma((3,)), dma((rows,)), dma((rows,)), dma, dma((len(cuts), 2)), dma((len(cuts), sp_size)),
                dma((sp_size,)), dma((sp_size,)), dma((groups, sp_size)), dma((groups, sp_size)),
                dma((5, len(cuts), sp_size)), dma((5, len(cuts), sp_size)),
            ],
            compiler_params=pltpu.CompilerParams(vmem_limit_bytes=46 * 2 ** 20, collective_id=0, has_side_effects=True),
            cost_estimate=pl.CostEstimate(flops=10 ** 9, bytes_accessed=42 * 10 ** 6, transcendentals=0),
            name="layer",
        )(*map(in_hbm, (positions, tokens, attn_gain.reshape(depth // 128, 128), mlp_gain.reshape(depth // 128, 128),
                        w_q, w_k, w_v, cache_k, cache_v, w_o, w_gate, w_up, w_down)))

        new_k, new_v, out, _, _ = pl.pallas_call(
            functools.partial(write_kernel, sp_size),
            out_shape=[pltpu.HBM(cache_k.shape, BF16), pltpu.HBM(cache_v.shape, BF16), pltpu.HBM((rows, depth), BF16),
                       bf16(*flat_shape), bf16(*flat_shape)],
            in_specs=[pl.BlockSpec(memory_space=pltpu.SMEM)] + [vmem] * 5,
            out_specs=[hbm] * 3 + [vmem] * 2,
            scratch_shapes=[dma((rows,)), dma((rows,)), dma],
            input_output_aliases={1: 3, 2: 4},
            compiler_params=pltpu.CompilerParams(vmem_limit_bytes=4 * 2 ** 20),
            cost_estimate=pl.CostEstimate(flops=10 ** 9, bytes_accessed=17 * 10 ** 6, transcendentals=0),
            name="write",
        )(positions, *map(in_vmem, (k_here, v_here, k_row, v_row, out_here)))
        return out, new_k, new_v

    return jax.shard_map(local_step, mesh=mesh, in_specs=in_specs, out_specs=out_specs, check_vma=False)
```

```python
import math
import functools
import jax
import jax.numpy as jnp
from jax import lax
from jax.experimental import pallas as pl
from jax.experimental.pallas import tpu as pltpu
from jax.sharding import PartitionSpec as P

NORM_EPS = 1e-5
ROPE_THETA = 10000.0
MESH = pl.DeviceIdType.MESH
F32 = jnp.float32
BF16 = jnp.bfloat16


def rope_tables(positions, half):
    index = lax.broadcasted_iota(jnp.int32, (positions.shape[0], half), 1).astype(F32)
    angles = positions * jnp.exp(index * (-math.log(ROPE_THETA) / half))
    turns = jnp.floor(angles * (2.0 / math.pi) + 0.5)
    rest = ((angles - turns * 1.5703125) - turns * 4.837512969970703125e-4) - turns * 7.54978995489188216e-8
    square = rest * rest
    sine = rest + rest * square * (-1.0 / 6 + square * (1.0 / 120 + square * (-1.0 / 5040 + square * (1.0 / 362880))))
    cosine = 1.0 + square * (-0.5 + square * (1.0 / 24 + square * (-1.0 / 720 + square * (1.0 / 40320 - square * (1.0 / 3628800)))))
    quadrant = turns.astype(jnp.int32) & 3
    swap = (quadrant & 1) == 1
    cos_value = jnp.where(swap, sine, cosine)
    sin_value = jnp.where(swap, cosine, sine)
    return (jnp.where((quadrant == 1) | (quadrant == 2), -cos_value, cos_value),
            jnp.where(quadrant >= 2, -sin_value, sin_value))


def scaled_norm(wide, gain_ref):
    inv_rms = lax.rsqrt(jnp.mean(wide * wide, axis=-1, keepdims=True) + NORM_EPS)
    gain = gain_ref[...].astype(F32)
    pieces = [(wide[:, i * 128:(i + 1) * 128] * inv_rms * gain[i:i + 1]).astype(BF16) for i in range(wide.shape[1] // 128)]
    return jnp.concatenate(pieces, axis=1)


def exchange(axis, source, slots_ref, send_sem, recv_sem):
    me = lax.axis_index(axis)
    size = slots_ref[0].shape[0]
    dst, cols = slots_ref
    copies = []
    for i in range(size - 1):
        down, up = size - 1 - i, i
        low = jnp.where(down > me, down, down - 1)
        high = jnp.where(up < me, up, up + 1)
        peer = jnp.where(me < size // 2, low, high)
        copies.append((
            pltpu.make_async_remote_copy(
                src_ref=source, dst_ref=dst.at[(me,) + cols], send_sem=send_sem.at[peer], recv_sem=recv_sem.at[me],
                device_id={axis: peer}, device_id_type=MESH),
            pltpu.make_async_remote_copy(
                src_ref=source, dst_ref=dst.at[(peer,) + cols], send_sem=send_sem.at[peer], recv_sem=recv_sem.at[peer],
                device_id={axis: peer}, device_id_type=MESH)))
        copies[-1][0].start()
    return copies


def finish(copies):
    for sent, arriving in copies:
        arriving.wait_recv()
    for sent, arriving in copies:
        sent.wait_send()


def added(slots_ref, cols):
    total = slots_ref[0, :, cols]
    for t in range(1, slots_ref.shape[0]):
        total = total + slots_ref[t, :, cols]
    return total


def layer_kernel(sp_size, tp_size, cuts, positions, tokens, attn_gain, mlp_gain, wq, wk, wv, ck, cv, wo, wg, wu, wd,
                 kbuf, vbuf, k_row, v_row, out_ref,
                 pos_ref, tok_ref, tok_cols, ag_ref, mg_ref, wqkv_buf, wo_buf, wgu_buf, wd_buf,
                 part0, r0, q3, k3, v3, kq3, vq3, o3, m3, l3, part1, r1, att, part2, r2, part3, r3, part4, r4, part5, r5, part6, r6,
                 psem, wsem, ksem, vsem, osem, gsem, dsem, ssem0, rsem0, ssem1, rsem1, ssem, rsem):
    rows, depth = tokens.shape
    _, local_slots, kv_local, head_dim = ck.shape
    slots = local_slots * sp_size
    q_width, kv_width = wq.shape[1], wk.shape[1]
    heads = q_width // head_dim
    group = heads // kv_local
    half = head_dim // 2
    width = depth // sp_size
    q_cols, kv_cols = q_width // sp_size, kv_width // sp_size
    flat = local_slots * kv_local
    sp, tp = lax.axis_index("sp"), lax.axis_index("tp")
    first_slot = sp * local_slots
    start = pl.multiple_of(sp * width, 128)
    my_cols = pl.ds(start, width)
    pieces = [pl.ds(a, b - a) for a, b in zip((0,) + cuts[:-1], cuts)]

    barrier = pltpu.get_barrier_semaphore()
    for axis, me, size in (("sp", sp, sp_size), ("tp", tp, tp_size)):
        for d in range(1, size):
            pl.semaphore_signal(barrier, inc=1, device_id={axis: lax.rem(me + d, size)}, device_id_type=MESH)

    small = [pltpu.make_async_copy(tokens, tok_ref, psem.at[0]), pltpu.make_async_copy(attn_gain, ag_ref, psem.at[1]),
             pltpu.make_async_copy(positions, pos_ref, psem.at[2]), pltpu.make_async_copy(mlp_gain, mg_ref, psem.at[3]),
             pltpu.make_async_copy(tokens.at[:, my_cols], tok_cols, psem.at[4])]
    q_part = pl.ds(pl.multiple_of(sp * q_cols, 128), q_cols)
    kv_part = pl.ds(pl.multiple_of(sp * kv_cols, 128), kv_cols)
    qkv_loads = [pltpu.make_async_copy(wq.at[:, q_part], wqkv_buf.at[:, pl.ds(0, q_cols)], wsem.at[0]),
                 pltpu.make_async_copy(wk.at[:, kv_part], wqkv_buf.at[:, pl.ds(q_cols, kv_cols)], wsem.at[1]),
                 pltpu.make_async_copy(wv.at[:, kv_part], wqkv_buf.at[:, pl.ds(q_cols + kv_cols, kv_cols)], wsem.at[2])]
    k_flat, v_flat = ck.reshape(rows, flat, head_dim), cv.reshape(rows, flat, head_dim)
    k_in = [pltpu.make_async_copy(k_flat.at[b], kbuf.at[b], ksem.at[b]) for b in range(rows)]
    v_in = [pltpu.make_async_copy(v_flat.at[b], vbuf.at[b], vsem.at[b]) for b in range(rows)]
    o_load = pltpu.make_async_copy(wo.at[:, my_cols], wo_buf, osem)
    gate_loads, down_loads = [], []
    for i, piece in enumerate(pieces):
        cols = pl.ds(start + piece.start, piece.size)
        gate_loads.append([
            pltpu.make_async_copy(wg.at[:, cols], wgu_buf.at[:, pl.ds(2 * piece.start, piece.size)], gsem.at[i, 0]),
            pltpu.make_async_copy(wu.at[:, cols], wgu_buf.at[:, pl.ds(2 * piece.start + piece.size, piece.size)], gsem.at[i, 1])])
        down_loads.append([
            pltpu.make_async_copy(wd.at[pl.ds(s * width + piece.start, piece.size), my_cols],
                                  wd_buf.at[pl.ds(sp_size * piece.start + s * piece.size, piece.size), :], dsem.at[i, s])
            for s in range(sp_size)])
    for copy in small + qkv_loads:
        copy.start()
    for b in range(rows):
        k_in[b].start()
        v_in[b].start()
    o_load.start()
    for loads in gate_loads + down_loads:
        for copy in loads:
            copy.start()

    with jax.named_scope("small"):
        for copy in small:
            copy.wait()
        normed = scaled_norm(tok_ref[...].astype(F32), ag_ref)
    with jax.named_scope("wait_qkv"):
        for copy in qkv_loads:
            copy.wait()
    with jax.named_scope("qkv"):
        mine = jnp.dot(normed, wqkv_buf[...], preferred_element_type=F32)
        part0[...] = mine
    with jax.named_scope("barrier"):
        pl.semaphore_wait(barrier, sp_size + tp_size - 2)
    moved = exchange("sp", part0, (r0, ()), ssem0, rsem0)
    r0[sp] = mine

    row = lax.broadcasted_iota(jnp.int32, (rows, half), 0)
    position_rows = jnp.zeros((rows, half), F32)
    for b in range(rows):
        position_rows = jnp.where(row == b, pos_ref[b].astype(F32), position_rows)
    cos_table, sin_table = rope_tables(position_rows, half)
    scale = 1.0 / math.sqrt(head_dim)
    side = part1.shape[1]
    tall = side * heads
    column = lax.broadcasted_iota(jnp.int32, (tall, flat), 1)
    line = lax.broadcasted_iota(jnp.int32, (tall, flat), 0)
    own_head = lax.rem(column, kv_local) == lax.rem(line, heads) // group
    member = line // heads
    value_member = lax.broadcasted_iota(jnp.int32, (tall, head_dim), 0) // heads
    slot_ids = first_slot + column // kv_local
    with jax.named_scope("p0"):
        finish(moved)

    def rotate(a, b):
        return a * cos_table - b * sin_table, b * cos_table + a * sin_table

    def gathered(offset, size, index):
        s, at = index * half // size, index * half % size
        return r0[s, :, offset + at:offset + at + half]

    for j in range(heads):
        a, b = rotate(gathered(0, q_cols, 2 * j), gathered(0, q_cols, 2 * j + 1))
        q3[:, j, 0:half] = a
        q3[:, j, half:head_dim] = b
    for j in range(kv_local):
        a, b = rotate(gathered(q_cols, kv_cols, 2 * j), gathered(q_cols, kv_cols, 2 * j + 1))
        k3[:, j, 0:half] = a
        k3[:, j, half:head_dim] = b
        v3[:, j, 0:half] = gathered(q_cols + kv_cols, kv_cols, 2 * j)
        v3[:, j, half:head_dim] = gathered(q_cols + kv_cols, kv_cols, 2 * j + 1)
    k_row[...] = k3[...].astype(BF16)
    v_row[...] = v3[...].astype(BF16)

    k_rounded, v_rounded = k_row[...].astype(F32), v_row[...].astype(F32)
    for j in range(heads):
        kq3[:, j, :] = k_rounded[:, j // group, :]
        vq3[:, j, :] = v_rounded[:, j // group, :]

    sends = []
    lane = lax.broadcasted_iota(jnp.int32, (side, 128), 1) // 16
    for g in range(rows // side):
        members = range(g * side, (g + 1) * side)
        with jax.named_scope(f"kv{g}"):
            for b in members:
                k_in[b].wait()
                v_in[b].wait()
        target = jnp.zeros((tall, flat), jnp.int32)
        limit = jnp.zeros((tall, flat), jnp.int32)
        for i, b in enumerate(members):
            position = pos_ref[b]
            target = jnp.where(member == i, lax.rem(position, slots), target)
            limit = jnp.where(member == i, jnp.where(position >= slots - 1, slots, position), limit)
        queries = jnp.concatenate([q3[b] for b in members], axis=0).astype(BF16)
        new_key = jnp.concatenate([kq3[b] for b in members], axis=0)
        new_value = jnp.concatenate([vq3[b] for b in members], axis=0)
        new_score = jnp.sum(queries.astype(F32) * new_key, axis=1, keepdims=True) * scale
        scores = jnp.zeros((tall, flat), F32)
        for i, b in enumerate(members):
            product = lax.dot_general(queries, kbuf[b], (((1,), (1,)), ((), ())), preferred_element_type=F32)
            scores = jnp.where(member == i, product, scores)
        fresh = slot_ids == target
        valid = own_head & (slot_ids <= limit)
        scores = jnp.where(valid, jnp.where(fresh, new_score, scores * scale), -jnp.inf)
        top = jnp.max(scores, axis=1, keepdims=True)
        weights = jnp.exp(scores - jnp.where(top == -jnp.inf, 0.0, top))
        new_weight = jnp.sum(jnp.where(fresh, weights, 0.0), axis=1, keepdims=True)
        stored = (weights * jnp.where(fresh, 0.0, 1.0)).astype(BF16)
        value = jnp.zeros((tall, head_dim), F32)
        for i, b in enumerate(members):
            product = jnp.dot(stored, vbuf[b], preferred_element_type=F32)
            value = jnp.where(value_member == i, product, value)
        value = value + new_weight.astype(BF16).astype(F32) * new_value
        top = jnp.broadcast_to(top, (tall, 128))
        size = jnp.broadcast_to(jnp.sum(weights, axis=1, keepdims=True), (tall, 128))
        for i, b in enumerate(members):
            own = slice(i * heads, (i + 1) * heads)
            o3[b], m3[b], l3[b] = value[own], top[own], size[own]
        rows_here = pl.ds(g * side, side)
        stats = jnp.zeros((side, 128), F32)
        for j in range(heads):
            part1[g, :, j * head_dim:(j + 1) * head_dim] = o3[rows_here, j, :]
            stats = jnp.where(lane == j, m3[rows_here, j, :], stats)
            stats = jnp.where(lane == heads + j, l3[rows_here, j, :], stats)
        part1[g, :, q_width:q_width + 128] = stats
        sends.append(exchange("sp", part1.at[g], (r1, (g,)), ssem1.at[g], rsem1.at[g]))
        r1[sp, g] = part1[g]

    for g, copies in enumerate(sends):
        with jax.named_scope(f"p1_{g}"):
            finish(copies)
        stats = [r1[s, g, :, q_width:q_width + 128] for s in range(sp_size)]
        for j in range(heads):
            tops = [t[:, j * 16:j * 16 + 1] for t in stats]
            best = functools.reduce(jnp.maximum, tops)
            numerator = jnp.zeros((side, head_dim), F32)
            denominator = jnp.zeros((side, 1), F32)
            for s in range(sp_size):
                factor = jnp.exp(tops[s] - best)
                numerator = numerator + r1[s, g, :, j * head_dim:(j + 1) * head_dim] * factor
                denominator = denominator + stats[s][:, (heads + j) * 16:(heads + j) * 16 + 1] * factor
            att[g * side:(g + 1) * side, j * head_dim:(j + 1) * head_dim] = numerator / denominator
    attended = att[...].astype(BF16)

    def pass_on(axis, me, source, slots_ref, phase, i):
        piece = pieces[i]
        copies = exchange(axis, source.at[:, piece], (slots_ref, (slice(None), piece)), ssem.at[phase, i], rsem.at[phase, i])
        slots_ref[me, :, piece] = source[:, piece]
        return copies

    def settle(base, sent, slots_ref, target, target_slots, phase):
        passed = []
        for i, piece in enumerate(pieces):
            with jax.named_scope(f"tp{phase}_{i}"):
                finish(sent[i])
            target[:, piece] = (base[:, piece] + added(slots_ref, piece)).astype(BF16).astype(F32)
            passed.append(pass_on("sp", sp, target, target_slots, phase, i))
        return passed

    with jax.named_scope("wait_o"):
        o_load.wait()
    sent = []
    for i, piece in enumerate(pieces):
        part2[:, piece] = jnp.dot(attended, wo_buf[:, piece], preferred_element_type=F32)
        sent.append(pass_on("tp", tp, part2, r2, 0, i))
    part6[...] = tok_cols[...].astype(F32)
    passed = settle(part6, sent, r2, part3, r3, 1)
    with jax.named_scope("wait_w"):
        for loads in gate_loads + down_loads:
            for copy in loads:
                copy.wait()
    with jax.named_scope("p3"):
        for copies in passed:
            finish(copies)
    normed = scaled_norm(jnp.concatenate([r3[s] for s in range(sp_size)], axis=1), mg_ref)

    moved = []
    for i, piece in enumerate(pieces):
        both = jnp.dot(normed, wgu_buf[:, 2 * piece.start:2 * (piece.start + piece.size)], preferred_element_type=F32)
        gate, up = both[:, :piece.size], both[:, piece.size:]
        part4[:, piece] = (gate * jax.nn.sigmoid(gate) * up).astype(BF16).astype(F32)
        moved.append(pass_on("sp", sp, part4, r4, 2, i))
    total = None
    for i, piece in enumerate(pieces):
        with jax.named_scope(f"p4_{i}"):
            finish(moved[i])
        left = jnp.concatenate([r4[s, :, piece] for s in range(sp_size)], axis=1).astype(BF16)
        down = pl.ds(sp_size * piece.start, sp_size * piece.size)
        if i + 1 < len(pieces):
            product = jnp.dot(left, wd_buf[down, :], preferred_element_type=F32)
            total = product if total is None else total + product
    part5[...] = total
    sent = []
    for i, piece in enumerate(pieces):
        part5[:, piece] = part5[:, piece] + jnp.dot(left, wd_buf[down, piece], preferred_element_type=F32)
        sent.append(pass_on("tp", tp, part5, r5, 3, i))
    passed = settle(part3, sent, r5, part6, r6, 4)
    with jax.named_scope("p6"):
        for copies in passed:
            finish(copies)
    out_ref[...] = jnp.concatenate([r6[s] for s in range(sp_size)], axis=1).astype(BF16)


def write_kernel(sp_size, pos_ref, k_in, v_in, k_row, v_row, out_in, new_k, new_v, out_ref, kbuf, vbuf, ksem, vsem, osem):
    rows, local_slots, kv_local, head_dim = new_k.shape
    flat = local_slots * kv_local
    tile = 16
    first_slot = lax.axis_index("sp") * local_slots
    copies = [pltpu.make_async_copy(out_in, out_ref, osem)]
    k_flat, v_flat = new_k.reshape(rows, flat, head_dim), new_v.reshape(rows, flat, head_dim)
    for b in range(rows):
        target = lax.rem(pos_ref[b], local_slots * sp_size) - first_slot

        @pl.when((target >= 0) & (target < local_slots))
        def _():
            base = pl.multiple_of((target * kv_local) // tile * tile, tile)
            at = target * kv_local - base
            row = lax.broadcasted_iota(jnp.int32, (tile, head_dim), 0)
            for buf, fresh in ((kbuf, k_row), (vbuf, v_row)):
                block = buf[b, pl.ds(base, tile), :].astype(F32)
                pair = fresh[b].astype(F32)
                for h in range(kv_local):
                    block = jnp.where(row == at + h, pair[h:h + 1], block)
                buf[b, pl.ds(base, tile), :] = block.astype(BF16)

    for b in range(rows):
        copies.append(pltpu.make_async_copy(kbuf.at[b], k_flat.at[b], ksem.at[b]))
        copies.append(pltpu.make_async_copy(vbuf.at[b], v_flat.at[b], vsem.at[b]))
    for copy in copies:
        copy.start()
    for copy in copies:
        copy.wait()


def solution(mesh):
    sp_size, tp_size = mesh.shape["sp"], mesh.shape["tp"]
    cache_spec = P("dp", "sp", "tp", None)
    row_spec = P("dp", None)
    col_spec = P(None, "tp")
    in_specs = (row_spec, P("dp"), cache_spec, cache_spec, P(None), col_spec, col_spec, col_spec, P("tp", None), P(None), col_spec, col_spec, P("tp", None))
    out_specs = (row_spec, cache_spec, cache_spec)

    def local_step(tokens, positions, cache_k, cache_v, attn_gain, w_q, w_k, w_v, w_o, mlp_gain, w_gate, w_up, w_down):
        rows, depth = tokens.shape
        _, local_slots, kv_local, head_dim = cache_k.shape
        q_width, kv_width = w_q.shape[1], w_k.shape[1]
        heads = q_width // head_dim
        width = depth // sp_size
        cuts = (512, width)
        groups = 2
        flat_shape = (rows, local_slots * kv_local, head_dim)
        vmem = pl.BlockSpec(memory_space=pltpu.VMEM)
        hbm = pl.BlockSpec(memory_space=pltpu.HBM)
        dma = pltpu.SemaphoreType.DMA
        in_hbm = functools.partial(pltpu.with_memory_space_constraint, memory_space=pltpu.HBM)
        in_vmem = functools.partial(pltpu.with_memory_space_constraint, memory_space=pltpu.VMEM)
        f32 = lambda *shape: pltpu.VMEM(shape, F32)
        bf16 = lambda *shape: pltpu.VMEM(shape, BF16)
        qkv_cols = (q_width + 2 * kv_width) // sp_size
        packed = (groups, rows // groups, q_width + 128)
        k_here, v_here, k_row, v_row, out_here = pl.pallas_call(
            functools.partial(layer_kernel, sp_size, tp_size, cuts),
            out_shape=[bf16(*flat_shape), bf16(*flat_shape), bf16(rows, kv_local, head_dim), bf16(rows, kv_local, head_dim), bf16(rows, depth)],
            in_specs=[hbm] * 13,
            out_specs=[vmem] * 5,
            scratch_shapes=[
                pltpu.SMEM((rows,), jnp.int32), bf16(rows, depth), bf16(rows, width), bf16(depth // 128, 128), bf16(depth // 128, 128),
                bf16(depth, qkv_cols), bf16(q_width, width), bf16(depth, 2 * width), bf16(w_down.shape[0], width),
                f32(rows, qkv_cols), f32(sp_size, rows, qkv_cols),
                f32(rows, heads, head_dim), f32(rows, kv_local, head_dim), f32(rows, kv_local, head_dim),
                f32(rows, heads, head_dim), f32(rows, heads, head_dim), f32(rows, heads, head_dim), f32(rows, heads, 128), f32(rows, heads, 128),
                f32(*packed), f32(sp_size, *packed), f32(rows, q_width),
                f32(rows, width), f32(tp_size, rows, width), f32(rows, width), f32(sp_size, rows, width),
                f32(rows, width), f32(sp_size, rows, width), f32(rows, width), f32(tp_size, rows, width),
                f32(rows, width), f32(sp_size, rows, width),
                dma((5,)), dma((3,)), dma((rows,)), dma((rows,)), dma, dma((len(cuts), 2)), dma((len(cuts), sp_size)),
                dma((sp_size,)), dma((sp_size,)), dma((groups, sp_size)), dma((groups, sp_size)),
                dma((5, len(cuts), sp_size)), dma((5, len(cuts), sp_size)),
            ],
            compiler_params=pltpu.CompilerParams(vmem_limit_bytes=46 * 2 ** 20, collective_id=0, has_side_effects=True),
            cost_estimate=pl.CostEstimate(flops=10 ** 9, bytes_accessed=42 * 10 ** 6, transcendentals=0),
            name="layer",
        )(*map(in_hbm, (positions, tokens, attn_gain.reshape(depth // 128, 128), mlp_gain.reshape(depth // 128, 128),
                        w_q, w_k, w_v, cache_k, cache_v, w_o, w_gate, w_up, w_down)))

        new_k, new_v, out, _, _ = pl.pallas_call(
            functools.partial(write_kernel, sp_size),
            out_shape=[pltpu.HBM(cache_k.shape, BF16), pltpu.HBM(cache_v.shape, BF16), pltpu.HBM((rows, depth), BF16),
                       bf16(*flat_shape), bf16(*flat_shape)],
            in_specs=[pl.BlockSpec(memory_space=pltpu.SMEM)] + [vmem] * 5,
            out_specs=[hbm] * 3 + [vmem] * 2,
            scratch_shapes=[dma((rows,)), dma((rows,)), dma],
            input_output_aliases={1: 3, 2: 4},
            compiler_params=pltpu.CompilerParams(vmem_limit_bytes=4 * 2 ** 20),
            cost_estimate=pl.CostEstimate(flops=10 ** 9, bytes_accessed=17 * 10 ** 6, transcendentals=0),
            name="write",
        )(positions, *map(in_vmem, (k_here, v_here, k_row, v_row, out_here)))
        return out, new_k, new_v

    return jax.shard_map(local_step, mesh=mesh, in_specs=in_specs, out_specs=out_specs, check_vma=False)
```

```python
import math
import functools
import jax
import jax.numpy as jnp
from jax import lax
from jax.experimental import pallas as pl
from jax.experimental.pallas import tpu as pltpu
from jax.sharding import PartitionSpec as P

NORM_EPS = 1e-5
ROPE_THETA = 10000.0
MESH = pl.DeviceIdType.MESH
F32 = jnp.float32
BF16 = jnp.bfloat16


def rope_tables(positions, half):
    index = lax.broadcasted_iota(jnp.int32, (positions.shape[0], half), 1).astype(F32)
    angles = positions * jnp.exp(index * (-math.log(ROPE_THETA) / half))
    turns = jnp.floor(angles * (2.0 / math.pi) + 0.5)
    rest = ((angles - turns * 1.5703125) - turns * 4.837512969970703125e-4) - turns * 7.54978995489188216e-8
    square = rest * rest
    sine = rest + rest * square * (-1.0 / 6 + square * (1.0 / 120 + square * (-1.0 / 5040 + square * (1.0 / 362880))))
    cosine = 1.0 + square * (-0.5 + square * (1.0 / 24 + square * (-1.0 / 720 + square * (1.0 / 40320 - square * (1.0 / 3628800)))))
    quadrant = turns.astype(jnp.int32) & 3
    swap = (quadrant & 1) == 1
    cos_value = jnp.where(swap, sine, cosine)
    sin_value = jnp.where(swap, cosine, sine)
    return (jnp.where((quadrant == 1) | (quadrant == 2), -cos_value, cos_value),
            jnp.where(quadrant >= 2, -sin_value, sin_value))


def scaled_norm(wide, gain_ref):
    inv_rms = lax.rsqrt(jnp.mean(wide * wide, axis=-1, keepdims=True) + NORM_EPS)
    gain = gain_ref[...].astype(F32)
    pieces = [(wide[:, i * 128:(i + 1) * 128] * inv_rms * gain[i:i + 1]).astype(BF16) for i in range(wide.shape[1] // 128)]
    return jnp.concatenate(pieces, axis=1)


def exchange(axis, source, slots_ref, send_sem, recv_sem, unsent):
    me = lax.axis_index(axis)
    size = slots_ref[0].shape[0]
    dst, cols = slots_ref
    copies = []
    for i in range(size - 1):
        down, up = size - 1 - i, i
        low = jnp.where(down > me, down, down - 1)
        high = jnp.where(up < me, up, up + 1)
        peer = jnp.where(me < size // 2, low, high)
        copies.append((
            pltpu.make_async_remote_copy(
                src_ref=source, dst_ref=dst.at[(me,) + cols], send_sem=send_sem.at[peer], recv_sem=recv_sem.at[me],
                device_id={axis: peer}, device_id_type=MESH),
            pltpu.make_async_remote_copy(
                src_ref=source, dst_ref=dst.at[(peer,) + cols], send_sem=send_sem.at[peer], recv_sem=recv_sem.at[peer],
                device_id={axis: peer}, device_id_type=MESH)))
        copies[-1][0].start()
    unsent.extend(sent for sent, _ in copies)
    return copies


def finish(copies):
    for _, arriving in copies:
        arriving.wait_recv()


def added(slots_ref, cols):
    total = slots_ref[0, :, cols]
    for t in range(1, slots_ref.shape[0]):
        total = total + slots_ref[t, :, cols]
    return total


def layer_kernel(sp_size, tp_size, cuts, positions, tokens, attn_gain, mlp_gain, wq, wk, wv, ck, cv, wo, wg, wu, wd,
                 kbuf, vbuf, k_row, v_row, out_ref,
                 pos_ref, tok_ref, tok_cols, ag_ref, mg_ref, wqkv_buf, wo_buf, wgu_buf, wd_buf,
                 part0, r0, q3, k3, v3, kq3, vq3, o3, m3, l3, part1, r1, att, part2, r2, part3, r3, part4, r4, part5, r5, part6, r6,
                 psem, wsem, ksem, vsem, osem, gsem, dsem, ssem0, rsem0, ssem1, rsem1, ssem, rsem):
    rows, depth = tokens.shape
    _, local_slots, kv_local, head_dim = ck.shape
    slots = local_slots * sp_size
    q_width, kv_width = wq.shape[1], wk.shape[1]
    heads = q_width // head_dim
    group = heads // kv_local
    half = head_dim // 2
    width = depth // sp_size
    q_cols, kv_cols = q_width // sp_size, kv_width // sp_size
    flat = local_slots * kv_local
    sp, tp = lax.axis_index("sp"), lax.axis_index("tp")
    first_slot = sp * local_slots
    start = pl.multiple_of(sp * width, 128)
    my_cols = pl.ds(start, width)
    cuts, mid_cuts = cuts
    pieces = [pl.ds(a, b - a) for a, b in zip((0,) + cuts[:-1], cuts)]
    mid_pieces = [pl.ds(a, b - a) for a, b in zip((0,) + mid_cuts[:-1], mid_cuts)]
    unsent = []

    barrier = pltpu.get_barrier_semaphore()
    for axis, me, size in (("sp", sp, sp_size), ("tp", tp, tp_size)):
        for d in range(1, size):
            pl.semaphore_signal(barrier, inc=1, device_id={axis: lax.rem(me + d, size)}, device_id_type=MESH)

    small = [pltpu.make_async_copy(tokens, tok_ref, psem.at[0]), pltpu.make_async_copy(attn_gain, ag_ref, psem.at[1]),
             pltpu.make_async_copy(positions, pos_ref, psem.at[2]), pltpu.make_async_copy(mlp_gain, mg_ref, psem.at[3]),
             pltpu.make_async_copy(tokens.at[:, my_cols], tok_cols, psem.at[4])]
    q_part = pl.ds(pl.multiple_of(sp * q_cols, 128), q_cols)
    kv_part = pl.ds(pl.multiple_of(sp * kv_cols, 128), kv_cols)
    qkv_loads = [pltpu.make_async_copy(wq.at[:, q_part], wqkv_buf.at[:, pl.ds(0, q_cols)], wsem.at[0]),
                 pltpu.make_async_copy(wk.at[:, kv_part], wqkv_buf.at[:, pl.ds(q_cols, kv_cols)], wsem.at[1]),
                 pltpu.make_async_copy(wv.at[:, kv_part], wqkv_buf.at[:, pl.ds(q_cols + kv_cols, kv_cols)], wsem.at[2])]
    k_flat, v_flat = ck.reshape(rows, flat, head_dim), cv.reshape(rows, flat, head_dim)
    k_in = [pltpu.make_async_copy(k_flat.at[b], kbuf.at[b], ksem.at[b]) for b in range(rows)]
    v_in = [pltpu.make_async_copy(v_flat.at[b], vbuf.at[b], vsem.at[b]) for b in range(rows)]
    o_load = pltpu.make_async_copy(wo.at[:, my_cols], wo_buf, osem)
    gate_loads, down_loads = [], []
    for i, piece in enumerate(mid_pieces):
        cols = pl.ds(start + piece.start, piece.size)
        gate_loads.append([
            pltpu.make_async_copy(wg.at[:, cols], wgu_buf.at[:, pl.ds(2 * piece.start, piece.size)], gsem.at[i, 0]),
            pltpu.make_async_copy(wu.at[:, cols], wgu_buf.at[:, pl.ds(2 * piece.start + piece.size, piece.size)], gsem.at[i, 1])])
        down_loads.append([
            pltpu.make_async_copy(wd.at[pl.ds(s * width + piece.start, piece.size), my_cols],
                                  wd_buf.at[pl.ds(sp_size * piece.start + s * piece.size, piece.size), :], dsem.at[i, s])
            for s in range(sp_size)])
    for copy in small[:2] + qkv_loads + small[2:]:
        copy.start()
    for b in range(rows):
        k_in[b].start()
        v_in[b].start()
    o_load.start()
    for loads in gate_loads + down_loads:
        for copy in loads:
            copy.start()

    with jax.named_scope("small"):
        for copy in small[:2]:
            copy.wait()
        normed = scaled_norm(tok_ref[...].astype(F32), ag_ref)
    with jax.named_scope("wait_qkv"):
        for copy in qkv_loads:
            copy.wait()
    with jax.named_scope("qkv"):
        mine = jnp.dot(normed, wqkv_buf[...], preferred_element_type=F32)
        part0[...] = mine
    with jax.named_scope("barrier"):
        pl.semaphore_wait(barrier, sp_size + tp_size - 2)
    moved = exchange("sp", part0, (r0, ()), ssem0, rsem0, unsent)
    r0[sp] = mine

    for copy in small[2:]:
        copy.wait()
    row = lax.broadcasted_iota(jnp.int32, (rows, half), 0)
    position_rows = jnp.zeros((rows, half), F32)
    for b in range(rows):
        position_rows = jnp.where(row == b, pos_ref[b].astype(F32), position_rows)
    cos_table, sin_table = rope_tables(position_rows, half)
    scale = 1.0 / math.sqrt(head_dim)
    side = part1.shape[1]
    tall = side * heads
    column = lax.broadcasted_iota(jnp.int32, (tall, flat), 1)
    line = lax.broadcasted_iota(jnp.int32, (tall, flat), 0)
    own_head = lax.rem(column, kv_local) == lax.rem(line, heads) // group
    member = line // heads
    value_member = lax.broadcasted_iota(jnp.int32, (tall, head_dim), 0) // heads
    slot_ids = first_slot + column // kv_local
    with jax.named_scope("p0"):
        finish(moved)

    def rotate(a, b):
        return a * cos_table - b * sin_table, b * cos_table + a * sin_table

    def gathered(offset, size, index):
        s, at = index * half // size, index * half % size
        return r0[s, :, offset + at:offset + at + half]

    for j in range(heads):
        a, b = rotate(gathered(0, q_cols, 2 * j), gathered(0, q_cols, 2 * j + 1))
        q3[:, j, 0:half] = a
        q3[:, j, half:head_dim] = b
    for j in range(kv_local):
        a, b = rotate(gathered(q_cols, kv_cols, 2 * j), gathered(q_cols, kv_cols, 2 * j + 1))
        k3[:, j, 0:half] = a
        k3[:, j, half:head_dim] = b
        v3[:, j, 0:half] = gathered(q_cols + kv_cols, kv_cols, 2 * j)
        v3[:, j, half:head_dim] = gathered(q_cols + kv_cols, kv_cols, 2 * j + 1)
    k_row[...] = k3[...].astype(BF16)
    v_row[...] = v3[...].astype(BF16)

    k_rounded, v_rounded = k_row[...].astype(F32), v_row[...].astype(F32)
    for j in range(heads):
        kq3[:, j, :] = k_rounded[:, j // group, :]
        vq3[:, j, :] = v_rounded[:, j // group, :]

    sends = []
    lane = lax.broadcasted_iota(jnp.int32, (side, 128), 1) // 16
    for g in range(rows // side):
        members = range(g * side, (g + 1) * side)
        with jax.named_scope(f"kv{g}"):
            for b in members:
                k_in[b].wait()
                v_in[b].wait()
        target = jnp.zeros((tall, flat), jnp.int32)
        limit = jnp.zeros((tall, flat), jnp.int32)
        for i, b in enumerate(members):
            position = pos_ref[b]
            target = jnp.where(member == i, lax.rem(position, slots), target)
            limit = jnp.where(member == i, jnp.where(position >= slots - 1, slots, position), limit)
        queries = jnp.concatenate([q3[b] for b in members], axis=0).astype(BF16)
        new_key = jnp.concatenate([kq3[b] for b in members], axis=0)
        new_value = jnp.concatenate([vq3[b] for b in members], axis=0)
        new_score = jnp.sum(queries.astype(F32) * new_key, axis=1, keepdims=True) * scale
        scores = jnp.zeros((tall, flat), F32)
        for i, b in enumerate(members):
            product = lax.dot_general(queries, kbuf[b], (((1,), (1,)), ((), ())), preferred_element_type=F32)
            scores = jnp.where(member == i, product, scores)
        fresh = slot_ids == target
        valid = own_head & (slot_ids <= limit)
        scores = jnp.where(valid, jnp.where(fresh, new_score, scores * scale), -jnp.inf)
        top = jnp.max(scores, axis=1, keepdims=True)
        weights = jnp.exp(scores - jnp.where(top == -jnp.inf, 0.0, top))
        new_weight = jnp.sum(jnp.where(fresh, weights, 0.0), axis=1, keepdims=True)
        stored = (weights * jnp.where(fresh, 0.0, 1.0)).astype(BF16)
        value = jnp.zeros((tall, head_dim), F32)
        for i, b in enumerate(members):
            product = jnp.dot(stored, vbuf[b], preferred_element_type=F32)
            value = jnp.where(value_member == i, product, value)
        value = value + new_weight.astype(BF16).astype(F32) * new_value
        top = jnp.broadcast_to(top, (tall, 128))
        size = jnp.broadcast_to(jnp.sum(weights, axis=1, keepdims=True), (tall, 128))
        for i, b in enumerate(members):
            own = slice(i * heads, (i + 1) * heads)
            o3[b], m3[b], l3[b] = value[own], top[own], size[own]
        rows_here = pl.ds(g * side, side)
        stats = jnp.zeros((side, 128), F32)
        for j in range(heads):
            part1[g, :, j * head_dim:(j + 1) * head_dim] = o3[rows_here, j, :]
            stats = jnp.where(lane == j, m3[rows_here, j, :], stats)
            stats = jnp.where(lane == heads + j, l3[rows_here, j, :], stats)
        part1[g, :, q_width:q_width + 128] = stats
        sends.append(exchange("sp", part1.at[g], (r1, (g,)), ssem1.at[g], rsem1.at[g], unsent))
        r1[sp, g] = part1[g]

    for g, copies in enumerate(sends):
        with jax.named_scope(f"p1_{g}"):
            finish(copies)
        stats = [r1[s, g, :, q_width:q_width + 128] for s in range(sp_size)]
        for j in range(heads):
            tops = [t[:, j * 16:j * 16 + 1] for t in stats]
            best = functools.reduce(jnp.maximum, tops)
            numerator = jnp.zeros((side, head_dim), F32)
            denominator = jnp.zeros((side, 1), F32)
            for s in range(sp_size):
                factor = jnp.exp(tops[s] - best)
                numerator = numerator + r1[s, g, :, j * head_dim:(j + 1) * head_dim] * factor
                denominator = denominator + stats[s][:, (heads + j) * 16:(heads + j) * 16 + 1] * factor
            att[g * side:(g + 1) * side, j * head_dim:(j + 1) * head_dim] = numerator / denominator
    attended = att[...].astype(BF16)

    def pass_on(axis, me, source, slots_ref, phase, i, piece):
        copies = exchange(axis, source.at[:, piece], (slots_ref, (slice(None), piece)), ssem.at[phase, i], rsem.at[phase, i], unsent)
        slots_ref[me, :, piece] = source[:, piece]
        return copies

    def settle(base, sent, slots_ref, target, target_slots, phase):
        passed = []
        for i, piece in enumerate(pieces):
            with jax.named_scope(f"tp{phase}_{i}"):
                finish(sent[i])
            target[:, piece] = (base[:, piece] + added(slots_ref, piece)).astype(BF16).astype(F32)
            passed.append(pass_on("sp", sp, target, target_slots, phase, i, piece))
        return passed

    o_load.wait()
    sent = []
    for i, piece in enumerate(pieces):
        with jax.named_scope(f"fence_o{i}"):
            unsent.pop(0).wait_send()
        part2[:, piece] = jnp.dot(attended, wo_buf[:, piece], preferred_element_type=F32)
        sent.append(pass_on("tp", tp, part2, r2, 0, i, piece))
    part6[...] = tok_cols[...].astype(F32)
    passed = settle(part6, sent, r2, part3, r3, 1)
    with jax.named_scope("p3"):
        for copies in passed:
            finish(copies)
    normed = scaled_norm(jnp.concatenate([r3[s] for s in range(sp_size)], axis=1), mg_ref)

    moved = []
    for i, piece in enumerate(mid_pieces):
        with jax.named_scope(f"wait_gate{i}"):
            for copy in gate_loads[i]:
                copy.wait()
        both = jnp.dot(normed, wgu_buf[:, 2 * piece.start:2 * (piece.start + piece.size)], preferred_element_type=F32)
        gate, up = both[:, :piece.size], both[:, piece.size:]
        part4[:, piece] = (gate * jax.nn.sigmoid(gate) * up).astype(BF16).astype(F32)
        moved.append(pass_on("sp", sp, part4, r4, 2, i, piece))
    total = None
    for i, piece in enumerate(mid_pieces):
        with jax.named_scope(f"p4_{i}"):
            for copy in down_loads[i]:
                copy.wait()
            finish(moved[i])
        left = jnp.concatenate([r4[s, :, piece] for s in range(sp_size)], axis=1).astype(BF16)
        down = pl.ds(sp_size * piece.start, sp_size * piece.size)
        if i + 1 < len(mid_pieces):
            product = jnp.dot(left, wd_buf[down, :], preferred_element_type=F32)
            total = product if total is None else total + product
            part5[...] = total
    sent = []
    for i, piece in enumerate(pieces):
        with jax.named_scope(f"fence{i}"):
            unsent.pop(0).wait_send()
        part5[:, piece] = part5[:, piece] + jnp.dot(left, wd_buf[down, piece], preferred_element_type=F32)
        sent.append(pass_on("tp", tp, part5, r5, 3, i, piece))
    passed = settle(part3, sent, r5, part6, r6, 4)
    with jax.named_scope("p6"):
        for copies in passed:
            finish(copies)
    for copy in unsent:
        copy.wait_send()
    out_ref[...] = jnp.concatenate([r6[s] for s in range(sp_size)], axis=1).astype(BF16)


def write_kernel(sp_size, pos_ref, k_in, v_in, k_row, v_row, out_in, new_k, new_v, out_ref, kbuf, vbuf, ksem, vsem, osem):
    rows, local_slots, kv_local, head_dim = new_k.shape
    flat = local_slots * kv_local
    tile = 16
    first_slot = lax.axis_index("sp") * local_slots
    copies = [pltpu.make_async_copy(out_in, out_ref, osem)]
    k_flat, v_flat = new_k.reshape(rows, flat, head_dim), new_v.reshape(rows, flat, head_dim)
    for b in range(rows):
        target = lax.rem(pos_ref[b], local_slots * sp_size) - first_slot

        @pl.when((target >= 0) & (target < local_slots))
        def _():
            base = pl.multiple_of((target * kv_local) // tile * tile, tile)
            at = target * kv_local - base
            row = lax.broadcasted_iota(jnp.int32, (tile, head_dim), 0)
            for buf, fresh in ((kbuf, k_row), (vbuf, v_row)):
                block = buf[b, pl.ds(base, tile), :].astype(F32)
                pair = fresh[b].astype(F32)
                for h in range(kv_local):
                    block = jnp.where(row == at + h, pair[h:h + 1], block)
                buf[b, pl.ds(base, tile), :] = block.astype(BF16)

    for b in range(rows):
        copies.append(pltpu.make_async_copy(kbuf.at[b], k_flat.at[b], ksem.at[b]))
        copies.append(pltpu.make_async_copy(vbuf.at[b], v_flat.at[b], vsem.at[b]))
    for copy in copies:
        copy.start()
    for copy in copies:
        copy.wait()


def solution(mesh):
    sp_size, tp_size = mesh.shape["sp"], mesh.shape["tp"]
    cache_spec = P("dp", "sp", "tp", None)
    row_spec = P("dp", None)
    col_spec = P(None, "tp")
    in_specs = (row_spec, P("dp"), cache_spec, cache_spec, P(None), col_spec, col_spec, col_spec, P("tp", None), P(None), col_spec, col_spec, P("tp", None))
    out_specs = (row_spec, cache_spec, cache_spec)

    def local_step(tokens, positions, cache_k, cache_v, attn_gain, w_q, w_k, w_v, w_o, mlp_gain, w_gate, w_up, w_down):
        rows, depth = tokens.shape
        _, local_slots, kv_local, head_dim = cache_k.shape
        q_width, kv_width = w_q.shape[1], w_k.shape[1]
        heads = q_width // head_dim
        width = depth // sp_size
        cuts = ((512, width), (512, width))
        groups = 2
        flat_shape = (rows, local_slots * kv_local, head_dim)
        vmem = pl.BlockSpec(memory_space=pltpu.VMEM)
        hbm = pl.BlockSpec(memory_space=pltpu.HBM)
        dma = pltpu.SemaphoreType.DMA
        in_hbm = functools.partial(pltpu.with_memory_space_constraint, memory_space=pltpu.HBM)
        in_vmem = functools.partial(pltpu.with_memory_space_constraint, memory_space=pltpu.VMEM)
        f32 = lambda *shape: pltpu.VMEM(shape, F32)
        bf16 = lambda *shape: pltpu.VMEM(shape, BF16)
        qkv_cols = (q_width + 2 * kv_width) // sp_size
        packed = (groups, rows // groups, q_width + 128)
        k_here, v_here, k_row, v_row, out_here = pl.pallas_call(
            functools.partial(layer_kernel, sp_size, tp_size, cuts),
            out_shape=[bf16(*flat_shape), bf16(*flat_shape), bf16(rows, kv_local, head_dim), bf16(rows, kv_local, head_dim), bf16(rows, depth)],
            in_specs=[hbm] * 13,
            out_specs=[vmem] * 5,
            scratch_shapes=[
                pltpu.SMEM((rows,), jnp.int32), bf16(rows, depth), bf16(rows, width), bf16(depth // 128, 128), bf16(depth // 128, 128),
                bf16(depth, qkv_cols), bf16(q_width, width), bf16(depth, 2 * width), bf16(w_down.shape[0], width),
                f32(rows, qkv_cols), f32(sp_size, rows, qkv_cols),
                f32(rows, heads, head_dim), f32(rows, kv_local, head_dim), f32(rows, kv_local, head_dim),
                f32(rows, heads, head_dim), f32(rows, heads, head_dim), f32(rows, heads, head_dim), f32(rows, heads, 128), f32(rows, heads, 128),
                f32(*packed), f32(sp_size, *packed), f32(rows, q_width),
                f32(rows, width), f32(tp_size, rows, width), f32(rows, width), f32(sp_size, rows, width),
                f32(rows, width), f32(sp_size, rows, width), f32(rows, width), f32(tp_size, rows, width),
                f32(rows, width), f32(sp_size, rows, width),
                dma((5,)), dma((3,)), dma((rows,)), dma((rows,)), dma, dma((2, 2)), dma((2, sp_size)),
                dma((sp_size,)), dma((sp_size,)), dma((groups, sp_size)), dma((groups, sp_size)),
                dma((5, 2, sp_size)), dma((5, 2, sp_size)),
            ],
            compiler_params=pltpu.CompilerParams(vmem_limit_bytes=46 * 2 ** 20, collective_id=0, has_side_effects=True),
            cost_estimate=pl.CostEstimate(flops=10 ** 9, bytes_accessed=42 * 10 ** 6, transcendentals=0),
            name="layer",
        )(*map(in_hbm, (positions, tokens, attn_gain.reshape(depth // 128, 128), mlp_gain.reshape(depth // 128, 128),
                        w_q, w_k, w_v, cache_k, cache_v, w_o, w_gate, w_up, w_down)))

        new_k, new_v, out, _, _ = pl.pallas_call(
            functools.partial(write_kernel, sp_size),
            out_shape=[pltpu.HBM(cache_k.shape, BF16), pltpu.HBM(cache_v.shape, BF16), pltpu.HBM((rows, depth), BF16),
                       bf16(*flat_shape), bf16(*flat_shape)],
            in_specs=[pl.BlockSpec(memory_space=pltpu.SMEM)] + [vmem] * 5,
            out_specs=[hbm] * 3 + [vmem] * 2,
            scratch_shapes=[dma((rows,)), dma((rows,)), dma],
            input_output_aliases={1: 3, 2: 4},
            compiler_params=pltpu.CompilerParams(vmem_limit_bytes=4 * 2 ** 20),
            cost_estimate=pl.CostEstimate(flops=10 ** 9, bytes_accessed=17 * 10 ** 6, transcendentals=0),
            name="write",
        )(positions, *map(in_vmem, (k_here, v_here, k_row, v_row, out_here)))
        return out, new_k, new_v

    return jax.shard_map(local_step, mesh=mesh, in_specs=in_specs, out_specs=out_specs, check_vma=False)
```

```python
import math
import functools
import jax
import jax.numpy as jnp
from jax import lax
from jax.experimental import pallas as pl
from jax.experimental.pallas import tpu as pltpu
from jax.sharding import PartitionSpec as P

NORM_EPS = 1e-5
ROPE_THETA = 10000.0
MESH = pl.DeviceIdType.MESH
F32 = jnp.float32
BF16 = jnp.bfloat16


def rope_tables(positions, half):
    index = lax.broadcasted_iota(jnp.int32, (positions.shape[0], half), 1).astype(F32)
    angles = positions * jnp.exp(index * (-math.log(ROPE_THETA) / half))
    turns = jnp.floor(angles * (2.0 / math.pi) + 0.5)
    rest = ((angles - turns * 1.5703125) - turns * 4.837512969970703125e-4) - turns * 7.54978995489188216e-8
    square = rest * rest
    sine = rest + rest * square * (-1.0 / 6 + square * (1.0 / 120 + square * (-1.0 / 5040 + square * (1.0 / 362880))))
    cosine = 1.0 + square * (-0.5 + square * (1.0 / 24 + square * (-1.0 / 720 + square * (1.0 / 40320 - square * (1.0 / 3628800)))))
    quadrant = turns.astype(jnp.int32) & 3
    swap = (quadrant & 1) == 1
    cos_value = jnp.where(swap, sine, cosine)
    sin_value = jnp.where(swap, cosine, sine)
    return (jnp.where((quadrant == 1) | (quadrant == 2), -cos_value, cos_value),
            jnp.where(quadrant >= 2, -sin_value, sin_value))


def scaled_norm(wide, gain_ref):
    inv_rms = lax.rsqrt(jnp.mean(wide * wide, axis=-1, keepdims=True) + NORM_EPS)
    gain = gain_ref[...].astype(F32)
    pieces = [(wide[:, i * 128:(i + 1) * 128] * inv_rms * gain[i:i + 1]).astype(BF16) for i in range(wide.shape[1] // 128)]
    return jnp.concatenate(pieces, axis=1)


def exchange(axis, source, slots_ref, send_sem, recv_sem, unsent):
    me = lax.axis_index(axis)
    size = slots_ref[0].shape[0]
    dst, cols = slots_ref
    copies = []
    for i in range(size - 1):
        down, up = size - 1 - i, i
        low = jnp.where(down > me, down, down - 1)
        high = jnp.where(up < me, up, up + 1)
        peer = jnp.where(me < size // 2, low, high)
        copies.append((
            pltpu.make_async_remote_copy(
                src_ref=source, dst_ref=dst.at[(me,) + cols], send_sem=send_sem.at[peer], recv_sem=recv_sem.at[me],
                device_id={axis: peer}, device_id_type=MESH),
            pltpu.make_async_remote_copy(
                src_ref=source, dst_ref=dst.at[(peer,) + cols], send_sem=send_sem.at[peer], recv_sem=recv_sem.at[peer],
                device_id={axis: peer}, device_id_type=MESH)))
        copies[-1][0].start()
    unsent.extend(sent for sent, _ in copies)
    return copies


def finish(copies):
    for _, arriving in copies:
        arriving.wait_recv()


def added(slots_ref, cols):
    total = slots_ref[0, :, cols]
    for t in range(1, slots_ref.shape[0]):
        total = total + slots_ref[t, :, cols]
    return total


def layer_kernel(sp_size, tp_size, cuts, positions, tokens, attn_gain, mlp_gain, wq, wk, wv, ck, cv, wo, wg, wu, wd,
                 kbuf, vbuf, k_row, v_row, out_ref,
                 pos_ref, tok_ref, tok_cols, ag_ref, mg_ref, wqkv_buf, wo_buf, wgu_buf, wd_buf,
                 part0, r0, q3, k3, v3, kq3, vq3, o3, m3, l3, part1, r1, att, part2, r2, part3, r3, part4, r4, part5, r5, part6, r6,
                 psem, wsem, ksem, vsem, osem, gsem, dsem, ssem0, rsem0, ssem1, rsem1, ssem, rsem):
    rows, depth = tokens.shape
    _, local_slots, kv_local, head_dim = ck.shape
    slots = local_slots * sp_size
    q_width, kv_width = wq.shape[1], wk.shape[1]
    heads = q_width // head_dim
    group = heads // kv_local
    half = head_dim // 2
    width = depth // sp_size
    q_cols, kv_cols = q_width // sp_size, kv_width // sp_size
    flat = local_slots * kv_local
    sp, tp = lax.axis_index("sp"), lax.axis_index("tp")
    first_slot = sp * local_slots
    start = pl.multiple_of(sp * width, 128)
    my_cols = pl.ds(start, width)
    cuts, mid_cuts = cuts
    pieces = [pl.ds(a, b - a) for a, b in zip((0,) + cuts[:-1], cuts)]
    mid_pieces = [pl.ds(a, b - a) for a, b in zip((0,) + mid_cuts[:-1], mid_cuts)]
    unsent = []

    barrier = pltpu.get_barrier_semaphore()
    for axis, me, size in (("sp", sp, sp_size), ("tp", tp, tp_size)):
        for d in range(1, size):
            pl.semaphore_signal(barrier, inc=1, device_id={axis: lax.rem(me + d, size)}, device_id_type=MESH)

    small = [pltpu.make_async_copy(tokens, tok_ref, psem.at[0]), pltpu.make_async_copy(attn_gain, ag_ref, psem.at[1]),
             pltpu.make_async_copy(positions, pos_ref, psem.at[2]), pltpu.make_async_copy(mlp_gain, mg_ref, psem.at[3]),
             pltpu.make_async_copy(tokens.at[:, my_cols], tok_cols, psem.at[4])]
    q_part = pl.ds(pl.multiple_of(sp * q_cols, 128), q_cols)
    kv_part = pl.ds(pl.multiple_of(sp * kv_cols, 128), kv_cols)
    qkv_loads = [pltpu.make_async_copy(wq.at[:, q_part], wqkv_buf.at[:, pl.ds(0, q_cols)], wsem.at[0]),
                 pltpu.make_async_copy(wk.at[:, kv_part], wqkv_buf.at[:, pl.ds(q_cols, kv_cols)], wsem.at[1]),
                 pltpu.make_async_copy(wv.at[:, kv_part], wqkv_buf.at[:, pl.ds(q_cols + kv_cols, kv_cols)], wsem.at[2])]
    k_flat, v_flat = ck.reshape(rows, flat, head_dim), cv.reshape(rows, flat, head_dim)
    k_in = [pltpu.make_async_copy(k_flat.at[b], kbuf.at[b], ksem.at[b]) for b in range(rows)]
    v_in = [pltpu.make_async_copy(v_flat.at[b], vbuf.at[b], vsem.at[b]) for b in range(rows)]
    o_load = pltpu.make_async_copy(wo.at[:, my_cols], wo_buf, osem)
    gate_loads, down_loads = [], []
    for i, piece in enumerate(mid_pieces):
        cols = pl.ds(start + piece.start, piece.size)
        gate_loads.append([
            pltpu.make_async_copy(wg.at[:, cols], wgu_buf.at[:, pl.ds(2 * piece.start, piece.size)], gsem.at[i, 0]),
            pltpu.make_async_copy(wu.at[:, cols], wgu_buf.at[:, pl.ds(2 * piece.start + piece.size, piece.size)], gsem.at[i, 1])])
        down_loads.append([
            pltpu.make_async_copy(wd.at[pl.ds(s * width + piece.start, piece.size), my_cols],
                                  wd_buf.at[pl.ds(sp_size * piece.start + s * piece.size, piece.size), :], dsem.at[i, s])
            for s in range(sp_size)])
    for copy in small[:2] + qkv_loads + small[2:]:
        copy.start()
    for b in range(rows):
        k_in[b].start()
        v_in[b].start()
    o_load.start()
    for loads in gate_loads + down_loads:
        for copy in loads:
            copy.start()

    with jax.named_scope("small"):
        for copy in small[:2]:
            copy.wait()
        normed = scaled_norm(tok_ref[...].astype(F32), ag_ref)
    with jax.named_scope("wait_qkv"):
        for copy in qkv_loads:
            copy.wait()
    with jax.named_scope("qkv"):
        mine = jnp.dot(normed, wqkv_buf[...], preferred_element_type=F32)
        part0[...] = mine
    with jax.named_scope("barrier"):
        pl.semaphore_wait(barrier, sp_size + tp_size - 2)
    moved = exchange("sp", part0, (r0, ()), ssem0, rsem0, unsent)
    r0[sp] = mine

    for copy in small[2:]:
        copy.wait()
    row = lax.broadcasted_iota(jnp.int32, (rows, half), 0)
    position_rows = jnp.zeros((rows, half), F32)
    for b in range(rows):
        position_rows = jnp.where(row == b, pos_ref[b].astype(F32), position_rows)
    cos_table, sin_table = rope_tables(position_rows, half)
    scale = 1.0 / math.sqrt(head_dim)
    side = part1.shape[1]
    tall = side * heads
    column = lax.broadcasted_iota(jnp.int32, (tall, flat), 1)
    line = lax.broadcasted_iota(jnp.int32, (tall, flat), 0)
    own_head = lax.rem(column, kv_local) == lax.rem(line, heads) // group
    member = line // heads
    value_member = lax.broadcasted_iota(jnp.int32, (tall, head_dim), 0) // heads
    slot_ids = first_slot + column // kv_local
    with jax.named_scope("p0"):
        finish(moved)

    def rotate(a, b):
        return a * cos_table - b * sin_table, b * cos_table + a * sin_table

    def gathered(offset, size, index):
        s, at = index * half // size, index * half % size
        return r0[s, :, offset + at:offset + at + half]

    for j in range(heads):
        a, b = rotate(gathered(0, q_cols, 2 * j), gathered(0, q_cols, 2 * j + 1))
        q3[:, j, 0:half] = a
        q3[:, j, half:head_dim] = b
    for j in range(kv_local):
        a, b = rotate(gathered(q_cols, kv_cols, 2 * j), gathered(q_cols, kv_cols, 2 * j + 1))
        k3[:, j, 0:half] = a
        k3[:, j, half:head_dim] = b
        v3[:, j, 0:half] = gathered(q_cols + kv_cols, kv_cols, 2 * j)
        v3[:, j, half:head_dim] = gathered(q_cols + kv_cols, kv_cols, 2 * j + 1)
    k_row[...] = k3[...].astype(BF16)
    v_row[...] = v3[...].astype(BF16)

    k_rounded, v_rounded = k_row[...].astype(F32), v_row[...].astype(F32)
    for j in range(heads):
        kq3[:, j, :] = k_rounded[:, j // group, :]
        vq3[:, j, :] = v_rounded[:, j // group, :]

    sends = []
    lane = lax.broadcasted_iota(jnp.int32, (side, 128), 1) // 16
    for g in range(rows // side):
        members = range(g * side, (g + 1) * side)
        with jax.named_scope(f"kv{g}"):
            for b in members:
                k_in[b].wait()
                v_in[b].wait()
        target = jnp.zeros((tall, flat), jnp.int32)
        limit = jnp.zeros((tall, flat), jnp.int32)
        for i, b in enumerate(members):
            position = pos_ref[b]
            target = jnp.where(member == i, lax.rem(position, slots), target)
            limit = jnp.where(member == i, jnp.where(position >= slots - 1, slots, position), limit)
        queries = jnp.concatenate([q3[b] for b in members], axis=0).astype(BF16)
        new_key = jnp.concatenate([kq3[b] for b in members], axis=0)
        new_value = jnp.concatenate([vq3[b] for b in members], axis=0)
        new_score = jnp.sum(queries.astype(F32) * new_key, axis=1, keepdims=True) * scale
        scores = jnp.zeros((tall, flat), F32)
        for i, b in enumerate(members):
            product = lax.dot_general(queries, kbuf[b], (((1,), (1,)), ((), ())), preferred_element_type=F32)
            scores = jnp.where(member == i, product, scores)
        fresh = slot_ids == target
        valid = own_head & (slot_ids <= limit)
        scores = jnp.where(valid, jnp.where(fresh, new_score, scores * scale), -jnp.inf)
        top = jnp.max(scores, axis=1, keepdims=True)
        weights = jnp.exp(scores - jnp.where(top == -jnp.inf, 0.0, top))
        new_weight = jnp.sum(jnp.where(fresh, weights, 0.0), axis=1, keepdims=True)
        stored = (weights * jnp.where(fresh, 0.0, 1.0)).astype(BF16)
        value = jnp.zeros((tall, head_dim), F32)
        for i, b in enumerate(members):
            product = jnp.dot(stored, vbuf[b], preferred_element_type=F32)
            value = jnp.where(value_member == i, product, value)
        value = value + new_weight.astype(BF16).astype(F32) * new_value
        top = jnp.broadcast_to(top, (tall, 128))
        size = jnp.broadcast_to(jnp.sum(weights, axis=1, keepdims=True), (tall, 128))
        for i, b in enumerate(members):
            own = slice(i * heads, (i + 1) * heads)
            o3[b], m3[b], l3[b] = value[own], top[own], size[own]
        rows_here = pl.ds(g * side, side)
        stats = jnp.zeros((side, 128), F32)
        for j in range(heads):
            part1[g, :, j * head_dim:(j + 1) * head_dim] = o3[rows_here, j, :]
            stats = jnp.where(lane == j, m3[rows_here, j, :], stats)
            stats = jnp.where(lane == heads + j, l3[rows_here, j, :], stats)
        part1[g, :, q_width:q_width + 128] = stats
        sends.append(exchange("sp", part1.at[g], (r1, (g,)), ssem1.at[g], rsem1.at[g], unsent))
        r1[sp, g] = part1[g]

    for g, copies in enumerate(sends):
        with jax.named_scope(f"p1_{g}"):
            finish(copies)
        stats = [r1[s, g, :, q_width:q_width + 128] for s in range(sp_size)]
        for j in range(heads):
            tops = [t[:, j * 16:j * 16 + 1] for t in stats]
            best = functools.reduce(jnp.maximum, tops)
            numerator = jnp.zeros((side, head_dim), F32)
            denominator = jnp.zeros((side, 1), F32)
            for s in range(sp_size):
                factor = jnp.exp(tops[s] - best)
                numerator = numerator + r1[s, g, :, j * head_dim:(j + 1) * head_dim] * factor
                denominator = denominator + stats[s][:, (heads + j) * 16:(heads + j) * 16 + 1] * factor
            att[g * side:(g + 1) * side, j * head_dim:(j + 1) * head_dim] = numerator / denominator
    attended = att[...].astype(BF16)

    def pass_on(axis, me, source, slots_ref, phase, i, piece):
        copies = exchange(axis, source.at[:, piece], (slots_ref, (slice(None), piece)), ssem.at[phase, i], rsem.at[phase, i], unsent)
        slots_ref[me, :, piece] = source[:, piece]
        return copies

    def settle(base, sent, slots_ref, target, target_slots, phase):
        passed = []
        for i, piece in enumerate(pieces):
            with jax.named_scope(f"tp{phase}_{i}"):
                finish(sent[i])
            target[:, piece] = (base[:, piece] + added(slots_ref, piece)).astype(BF16).astype(F32)
            passed.append(pass_on("sp", sp, target, target_slots, phase, i, piece))
        return passed

    o_load.wait()
    sent = []
    for i, piece in enumerate(pieces):
        part2[:, piece] = jnp.dot(attended, wo_buf[:, piece], preferred_element_type=F32)
        sent.append(pass_on("tp", tp, part2, r2, 0, i, piece))
    part6[...] = tok_cols[...].astype(F32)
    passed = settle(part6, sent, r2, part3, r3, 1)
    with jax.named_scope("p3"):
        for copies in passed:
            finish(copies)
    normed = scaled_norm(jnp.concatenate([r3[s] for s in range(sp_size)], axis=1), mg_ref)

    moved = []
    for i, piece in enumerate(mid_pieces):
        with jax.named_scope(f"wait_gate{i}"):
            for copy in gate_loads[i]:
                copy.wait()
        both = jnp.dot(normed, wgu_buf[:, 2 * piece.start:2 * (piece.start + piece.size)], preferred_element_type=F32)
        gate, up = both[:, :piece.size], both[:, piece.size:]
        part4[:, piece] = (gate * jax.nn.sigmoid(gate) * up).astype(BF16).astype(F32)
        moved.append(pass_on("sp", sp, part4, r4, 2, i, piece))
    total = None
    for i, piece in enumerate(mid_pieces):
        with jax.named_scope(f"p4_{i}"):
            for copy in down_loads[i]:
                copy.wait()
            finish(moved[i])
        left = jnp.concatenate([r4[s, :, piece] for s in range(sp_size)], axis=1).astype(BF16)
        down = pl.ds(sp_size * piece.start, sp_size * piece.size)
        if i + 1 < len(mid_pieces):
            product = jnp.dot(left, wd_buf[down, :], preferred_element_type=F32)
            total = product if total is None else total + product
            part5[...] = total
    sent = []
    for i, piece in enumerate(pieces):
        part5[:, piece] = part5[:, piece] + jnp.dot(left, wd_buf[down, piece], preferred_element_type=F32)
        sent.append(pass_on("tp", tp, part5, r5, 3, i, piece))
    passed = settle(part3, sent, r5, part6, r6, 4)
    with jax.named_scope("p6"):
        for copies in passed:
            finish(copies)
    for copy in unsent:
        copy.wait_send()
    out_ref[...] = jnp.concatenate([r6[s] for s in range(sp_size)], axis=1).astype(BF16)


def write_kernel(sp_size, pos_ref, k_in, v_in, k_row, v_row, out_in, new_k, new_v, out_ref, kbuf, vbuf, ksem, vsem, osem):
    rows, local_slots, kv_local, head_dim = new_k.shape
    flat = local_slots * kv_local
    tile = 16
    first_slot = lax.axis_index("sp") * local_slots
    copies = [[pltpu.make_async_copy(out_in, out_ref, osem)]]
    k_flat, v_flat = new_k.reshape(rows, flat, head_dim), new_v.reshape(rows, flat, head_dim)
    for b in range(rows):
        target = lax.rem(pos_ref[b], local_slots * sp_size) - first_slot

        @pl.when((target >= 0) & (target < local_slots))
        def _():
            base = pl.multiple_of((target * kv_local) // tile * tile, tile)
            at = target * kv_local - base
            row = lax.broadcasted_iota(jnp.int32, (tile, head_dim), 0)
            for buf, fresh in ((kbuf, k_row), (vbuf, v_row)):
                block = buf[b, pl.ds(base, tile), :].astype(F32)
                pair = fresh[b].astype(F32)
                for h in range(kv_local):
                    block = jnp.where(row == at + h, pair[h:h + 1], block)
                buf[b, pl.ds(base, tile), :] = block.astype(BF16)

        copies.append([pltpu.make_async_copy(kbuf.at[b], k_flat.at[b], ksem.at[b]), pltpu.make_async_copy(vbuf.at[b], v_flat.at[b], vsem.at[b])])
        for copy in copies[b]:
            copy.start()
    for copy in copies[rows]:
        copy.start()
    for pair in copies:
        for copy in pair:
            copy.wait()


def solution(mesh):
    sp_size, tp_size = mesh.shape["sp"], mesh.shape["tp"]
    cache_spec = P("dp", "sp", "tp", None)
    row_spec = P("dp", None)
    col_spec = P(None, "tp")
    in_specs = (row_spec, P("dp"), cache_spec, cache_spec, P(None), col_spec, col_spec, col_spec, P("tp", None), P(None), col_spec, col_spec, P("tp", None))
    out_specs = (row_spec, cache_spec, cache_spec)

    def local_step(tokens, positions, cache_k, cache_v, attn_gain, w_q, w_k, w_v, w_o, mlp_gain, w_gate, w_up, w_down):
        rows, depth = tokens.shape
        _, local_slots, kv_local, head_dim = cache_k.shape
        q_width, kv_width = w_q.shape[1], w_k.shape[1]
        heads = q_width // head_dim
        width = depth // sp_size
        cuts = ((512, width), (512, width))
        groups = 2
        flat_shape = (rows, local_slots * kv_local, head_dim)
        vmem = pl.BlockSpec(memory_space=pltpu.VMEM)
        hbm = pl.BlockSpec(memory_space=pltpu.HBM)
        dma = pltpu.SemaphoreType.DMA
        in_hbm = functools.partial(pltpu.with_memory_space_constraint, memory_space=pltpu.HBM)
        in_vmem = functools.partial(pltpu.with_memory_space_constraint, memory_space=pltpu.VMEM)
        f32 = lambda *shape: pltpu.VMEM(shape, F32)
        bf16 = lambda *shape: pltpu.VMEM(shape, BF16)
        qkv_cols = (q_width + 2 * kv_width) // sp_size
        packed = (groups, rows // groups, q_width + 128)
        k_here, v_here, k_row, v_row, out_here = pl.pallas_call(
            functools.partial(layer_kernel, sp_size, tp_size, cuts),
            out_shape=[bf16(*flat_shape), bf16(*flat_shape), bf16(rows, kv_local, head_dim), bf16(rows, kv_local, head_dim), bf16(rows, depth)],
            in_specs=[hbm] * 13,
            out_specs=[vmem] * 5,
            scratch_shapes=[
                pltpu.SMEM((rows,), jnp.int32), bf16(rows, depth), bf16(rows, width), bf16(depth // 128, 128), bf16(depth // 128, 128),
                bf16(depth, qkv_cols), bf16(q_width, width), bf16(depth, 2 * width), bf16(w_down.shape[0], width),
                f32(rows, qkv_cols), f32(sp_size, rows, qkv_cols),
                f32(rows, heads, head_dim), f32(rows, kv_local, head_dim), f32(rows, kv_local, head_dim),
                f32(rows, heads, head_dim), f32(rows, heads, head_dim), f32(rows, heads, head_dim), f32(rows, heads, 128), f32(rows, heads, 128),
                f32(*packed), f32(sp_size, *packed), f32(rows, q_width),
                f32(rows, width), f32(tp_size, rows, width), f32(rows, width), f32(sp_size, rows, width),
                f32(rows, width), f32(sp_size, rows, width), f32(rows, width), f32(tp_size, rows, width),
                f32(rows, width), f32(sp_size, rows, width),
                dma((5,)), dma((3,)), dma((rows,)), dma((rows,)), dma, dma((2, 2)), dma((2, sp_size)),
                dma((sp_size,)), dma((sp_size,)), dma((groups, sp_size)), dma((groups, sp_size)),
                dma((5, 2, sp_size)), dma((5, 2, sp_size)),
            ],
            compiler_params=pltpu.CompilerParams(vmem_limit_bytes=46 * 2 ** 20, collective_id=0, has_side_effects=True),
            cost_estimate=pl.CostEstimate(flops=10 ** 9, bytes_accessed=42 * 10 ** 6, transcendentals=0),
            name="layer",
        )(*map(in_hbm, (positions, tokens, attn_gain.reshape(depth // 128, 128), mlp_gain.reshape(depth // 128, 128),
                        w_q, w_k, w_v, cache_k, cache_v, w_o, w_gate, w_up, w_down)))

        new_k, new_v, out, _, _ = pl.pallas_call(
            functools.partial(write_kernel, sp_size),
            out_shape=[pltpu.HBM(cache_k.shape, BF16), pltpu.HBM(cache_v.shape, BF16), pltpu.HBM((rows, depth), BF16),
                       bf16(*flat_shape), bf16(*flat_shape)],
            in_specs=[pl.BlockSpec(memory_space=pltpu.SMEM)] + [vmem] * 5,
            out_specs=[hbm] * 3 + [vmem] * 2,
            scratch_shapes=[dma((rows,)), dma((rows,)), dma],
            input_output_aliases={1: 3, 2: 4},
            compiler_params=pltpu.CompilerParams(vmem_limit_bytes=4 * 2 ** 20),
            cost_estimate=pl.CostEstimate(flops=10 ** 9, bytes_accessed=17 * 10 ** 6, transcendentals=0),
            name="write",
        )(positions, *map(in_vmem, (k_here, v_here, k_row, v_row, out_here)))
        return out, new_k, new_v

    return jax.shard_map(local_step, mesh=mesh, in_specs=in_specs, out_specs=out_specs, check_vma=False)
```
